256 devices in a mesh: rows: 32 (over y, x, core), grp: 8 (over z).
Axes of the slice: x: 4, y: 4, z: 8, core: 2. Of those that a mesh axis runs over, the one named last changes fastest.
Arguments:
- matrix: bfloat16 [131072, 2048], P(('rows', 'grp')), may hold values from -0.0625 to 0.0625
- right_side: bfloat16 [131072, 128], P(('rows', 'grp')), may hold values from -6 to 6
- precond: bfloat16 [2048, 2048], replicated, may hold values from -1 to 3
- row_counts: int32 [256], P(('rows', 'grp')), may hold values from 64 to 512, as said below
Outputs:
- solution: float32 [2048, 128], P(None, 'grp')
- coeffs: float32 [2048, 128], P(None, 'grp')
- rel_residual: float32 [128], P('grp')
The draws below stay inside these ranges and needn't reach their ends.
Inputs may be any that keep to these rules, and one draw needn't show every extreme that they name: Device d holds A's rows in its first row_counts[d] slots of 512; some device is full in every draw.
All inputs are finite; a program needn't handle non-finite values.
Results may differ from the reference program's by a relative error of at most 0.0128.
Values may be sent and summed in bfloat16 or wider, within the bound.
No kernel may reach another device: no remote copies, remote signals or barrier semaphores. Data moves between devices by JAX's collectives and lax.ppermute only.
A program may use at most 64 MiB of HBM per device.

```python
import math
import jax
import jax.numpy as jnp
from jax import lax

D = 2048
K = 128
ITERS = 3
R_DEV = 512
NDEV = 256
ROWS = 131072


def draw_row_counts(key, part):
    first, second = jax.random.split(key)
    base = jax.random.randint(first, (NDEV,), R_DEV // 8, R_DEV // 2 + 1, dtype=jnp.int32)
    fullest = jax.random.randint(second, (), 0, NDEV, dtype=jnp.int32)
    return jnp.where(jnp.arange(NDEV, dtype=jnp.int32) == fullest, R_DEV, base).astype(jnp.int32)


def draw_precond(key, part):
    first, second = jax.random.split(key)
    scales = jnp.exp(jax.random.uniform(first, (D,), minval=math.log(0.25), maxval=math.log(2.0)))
    noise = jax.random.normal(second, (D, D))
    return (jnp.diag(scales) + 0.5 * noise / math.sqrt(D)).astype(jnp.bfloat16)


def strengthened(values, stream_key, source, target, blocks, factor):
    def block_of(dim):
        return (jnp.arange(values.shape[dim]) // (values.shape[dim] // blocks)).reshape((-1,) + (1,) * (values.ndim - 1 - dim))

    near = jax.random.permutation(stream_key, blocks)[block_of(target)]
    second = (block_of(target) + blocks // 2) % blocks
    return jnp.where((block_of(source) == near) | (block_of(source) == second), factor * values, values)


def shard_levels(own_key, dims, shards, smallest, largest):
    def one(axis_at, blocks):
        steps = jax.random.uniform(jax.random.fold_in(jax.random.fold_in(own_key, 6), axis_at), (blocks,), jnp.float32, smallest / len(shards), largest / len(shards))
        return jnp.repeat(jnp.exp(steps), dims[axis_at] // blocks).reshape((-1,) + (1,) * (len(dims) - axis_at - 1))

    loudness = one(*shards[0])
    for cut in shards[1:]:
        loudness = loudness * one(*cut)
    return loudness


def normal_values(key, extent, width, reach, cuts=(), kind=jnp.bfloat16):
    loudness = shard_levels(key, extent, cuts, -0.22, 0.18) if cuts else 1.0
    values = jax.random.normal(key, extent, jnp.float32) * width * loudness
    return jnp.minimum(jnp.maximum(values, -reach), reach).astype(kind)


def noise_with(own_key, dims, width, reach, shards, heavy, kind=jnp.bfloat16):
    result = width * jax.random.normal(own_key, dims, jnp.float32)
    if shards:
        result = result * shard_levels(own_key, dims, shards, -0.22, 0.18)
    return jnp.clip(strengthened(result, jax.random.fold_in(own_key, 3), *heavy), -reach, reach).astype(kind)


def setup_inputs(seed: int = 0) -> dict:
    key_list = jax.random.split(jax.random.key(seed), 5)
    return {
        "matrix": noise_with(key_list[0], (ROWS, D), ROWS ** -0.5, 0.0625, ((0, 256),), (0, 1, 256, 6.0)),
        "right_side": normal_values(key_list[1], (ROWS, K), 1.0, 6.0, ((0, 256),)),
        "precond": draw_precond(jax.random.fold_in(key_list[4], 71), 0),
        "row_counts": draw_row_counts(jax.random.fold_in(key_list[4], 71), 0),
    }


floor_sq = 0.01

def pull_back(matrix, precond, residue):
    partial_value = lax.dot_general(matrix, residue.astype(jnp.bfloat16), (((0,), (0,)), ((), ())), preferred_element_type=jnp.float32)
    squares = lax.optimization_barrier(jnp.sum(residue * residue, axis=0, keepdims=True))
    u_norm = jnp.sqrt(squares + floor_sq)
    pulled = lax.dot_general(precond, (partial_value / u_norm).astype(jnp.bfloat16), (((0,), (0,)), ((), ())), preferred_element_type=jnp.float32)
    return (u_norm, pulled)

def reference(matrix, right_side, precond, row_counts):
    total_rows = matrix.shape[0]
    position = jnp.arange(total_rows, dtype=jnp.int32)
    owner = (position // R_DEV).astype(jnp.int32)
    live_rows = (position % R_DEV < row_counts[owner]).astype(jnp.float32)[:, None]
    residue = live_rows * right_side.astype(jnp.float32)
    u_norm, pulled = pull_back(matrix, precond, residue)
    v_norm = jnp.sqrt(lax.optimization_barrier(jnp.sum(pulled * pulled, axis=0, keepdims=True)) + floor_sq)
    right_vec = pulled / v_norm
    left_vec = residue / u_norm
    phi_bar = u_norm
    rho_bar = v_norm
    search = right_vec
    coeffs = jnp.zeros(right_vec.shape, jnp.float32)
    start_norm = u_norm
    for turn_index in range(ITERS):
        pushed = jnp.dot(precond, right_vec.astype(jnp.bfloat16), preferred_element_type=jnp.float32).astype(jnp.bfloat16)
        residue = live_rows * (jnp.dot(matrix, pushed, preferred_element_type=jnp.float32) - v_norm * left_vec)
        u_norm, pulled = pull_back(matrix, precond, residue)
        raw_vec = pulled - u_norm * right_vec
        next_norm = jnp.sqrt(lax.optimization_barrier(jnp.sum(raw_vec * raw_vec, axis=0, keepdims=True)) + floor_sq)
        next_vec = raw_vec / next_norm
        left_vec = residue / u_norm
        radius = jnp.sqrt(rho_bar * rho_bar + u_norm * u_norm)
        cosine = rho_bar / radius
        sine_part = u_norm / radius
        coupling = sine_part * next_norm
        rho_bar = -cosine * next_norm
        phi_step = cosine * phi_bar
        phi_bar = sine_part * phi_bar
        coeffs = coeffs + phi_step / radius * search
        search = next_vec - coupling / radius * search
        right_vec = next_vec
        v_norm = next_norm
    solution = jnp.dot(precond, coeffs.astype(jnp.bfloat16), preferred_element_type=jnp.float32)
    return (solution, coeffs, (phi_bar / start_norm)[0])
```

```python
import jax
import jax.numpy as jnp
from jax import lax
from jax.sharding import Mesh, PartitionSpec as P

ITERS = 3

floor_sq = 0.01
plane = ("y", "x")
every = ("y", "x", "core", "grp")
SQ_ROWS = 8


def split_terms(value):
    first = value.astype(jnp.bfloat16)
    rest = value - first.astype(jnp.float32)
    second = rest.astype(jnp.bfloat16)
    third = (rest - second.astype(jnp.float32)).astype(jnp.bfloat16)
    blank = jnp.zeros((SQ_ROWS - 3, value.shape[1]), jnp.bfloat16)
    return jnp.concatenate([first, second, third, blank])


def swap_cores(value):
    return lax.ppermute(value, "core", [(0, 1), (1, 0)])


def exchange(tiles, axis):
    return lax.all_to_all(tiles, axis, 0, 0, tiled=True)


def copies_from_all(value, axis):
    return exchange(jnp.broadcast_to(value, (lax.axis_size(axis), *value.shape)), axis)


def summed(tiles):
    return jnp.sum(tiles.astype(jnp.float32), axis=0)


def with_squares(tiles, squares):
    extra = jnp.broadcast_to(split_terms(squares), (tiles.shape[0], SQ_ROWS, tiles.shape[2]))
    return jnp.concatenate([tiles.astype(jnp.bfloat16), extra], axis=1)


def apart(block):
    return (block[:-SQ_ROWS], jnp.sum(block[-SQ_ROWS:], axis=0, keepdims=True))


def sum_everywhere(partial_value, squares):
    core = lax.axis_index("core")
    width, cols = partial_value.shape
    peers = lax.axis_size(plane)
    halves = partial_value.reshape(2, peers, width // 2 // peers, cols)
    mine = lax.dynamic_index_in_dim(halves, core, 0, keepdims=False)
    other = lax.dynamic_index_in_dim(halves, 1 - core, 0, keepdims=False)
    came = swap_cores(with_squares(other, squares)).astype(jnp.float32)
    came_rows, came_sq = (came[:, :-SQ_ROWS], jnp.sum(came[0, -SQ_ROWS:], axis=0, keepdims=True))
    block = summed(exchange(with_squares(mine + came_rows, squares + came_sq), plane))
    rows, squares = apart(block)
    block = summed(copies_from_all(with_squares(rows[None], squares)[0], "grp"))
    rows, squares = apart(block)
    half = copies_from_all(rows.astype(jnp.bfloat16), plane).reshape(width // 2, cols)
    twin = swap_cores(half)
    low = jnp.where(core == 0, half, twin)
    high = jnp.where(core == 0, twin, half)
    return (jnp.concatenate([low, high]), squares)


def sum_squares(squares):
    tiles = copies_from_all(squares, every)
    return jnp.sum(tiles, axis=0)


def pull(precond, total, squares):
    u_norm = jnp.sqrt(squares + floor_sq)
    pulled = lax.dot_general(
        precond, total, (((0,), (0,)), ((), ())), preferred_element_type=jnp.float32
    )
    return (u_norm, pulled / u_norm)


def shards(matrix, right_side, precond, row_counts):
    local_rows, width = matrix.shape
    count = row_counts[0]
    live_rows = (lax.broadcasted_iota(jnp.int32, (local_rows, 1), 0) < count).astype(jnp.float32)

    def partials(residue):
        partial_value = lax.dot_general(
            matrix,
            residue.astype(jnp.bfloat16),
            (((0,), (0,)), ((), ())),
            preferred_element_type=jnp.float32,
        )
        return (partial_value, jnp.sum(residue * residue, axis=0, keepdims=True))

    residue = live_rows * right_side.astype(jnp.float32)
    total, squares = sum_everywhere(*partials(residue))
    u_norm, raw_vec = pull(precond, total, squares)
    v_norm = jnp.sqrt(jnp.sum(raw_vec * raw_vec, axis=0, keepdims=True) + floor_sq)
    right_vec = raw_vec / v_norm
    phi_bar = u_norm
    rho_bar = v_norm
    search = right_vec
    coeffs = jnp.zeros(right_vec.shape, jnp.float32)
    solution = jnp.zeros(right_vec.shape, jnp.float32)
    search_image = None
    start_norm = u_norm
    for turn_index in range(ITERS):
        image = jnp.dot(
            precond, right_vec.astype(jnp.bfloat16), preferred_element_type=jnp.float32
        )
        search_image = image if search_image is None else image - step_back * search_image
        residue = live_rows * (
            jnp.dot(matrix, image.astype(jnp.bfloat16), preferred_element_type=jnp.float32)
            - v_norm * (residue / u_norm)
        )
        partial_value, squares = partials(residue)
        total, total_squares = sum_everywhere(partial_value, squares)
        if turn_index + 1 == ITERS:
            total_squares = sum_squares(squares)
        u_norm, pulled = pull(precond, total, total_squares)
        raw_vec = pulled - u_norm * right_vec
        next_norm = jnp.sqrt(jnp.sum(raw_vec * raw_vec, axis=0, keepdims=True) + floor_sq)
        next_vec = raw_vec / next_norm
        radius = jnp.sqrt(rho_bar * rho_bar + u_norm * u_norm)
        cosine = rho_bar / radius
        sine_part = u_norm / radius
        coupling = sine_part * next_norm
        rho_bar = -cosine * next_norm
        phi_step = cosine * phi_bar
        phi_bar = sine_part * phi_bar
        coeffs = coeffs + phi_step / radius * search
        solution = solution + phi_step / radius * search_image
        step_back = coupling / radius
        search = next_vec - step_back * search
        right_vec = next_vec
        v_norm = next_norm
    ratio = phi_bar / start_norm

    def own_columns(value):
        cols = value.shape[1] // lax.axis_size("grp")
        return lax.dynamic_slice_in_dim(value, lax.axis_index("grp") * cols, cols, axis=1)

    return (own_columns(solution), own_columns(coeffs), own_columns(ratio)[0])


def solution(mesh):
    fine = Mesh(mesh.devices.reshape(4, 4, 2, 8), every)
    return jax.shard_map(
        shards,
        mesh=fine,
        in_specs=(P(every, None), P(every, None), P(), P(every)),
        out_specs=(P(None, "grp"), P(None, "grp"), P("grp")),
        check_vma=False,
    )
```

```python
import functools

import jax
import jax.numpy as jnp
from jax import lax
from jax.experimental import pallas as pl
from jax.experimental.pallas import tpu as pltpu
from jax.sharding import Mesh, PartitionSpec as P

ITERS = 3

floor_sq = 0.01
plane = ("y", "x")
every = ("y", "x", "core", "grp")
SQ_ROWS = 8
LANES = 128
bf16, f32 = jnp.bfloat16, jnp.float32
VMEM = pl.BlockSpec(memory_space=pltpu.VMEM)
SMEM = pl.BlockSpec(memory_space=pltpu.SMEM)


def run(body, shapes, operands, specs, name, scratch=(), limit=None):
    return pl.pallas_call(
        body,
        out_shape=[jax.ShapeDtypeStruct(s, t) for s, t in shapes],
        in_specs=specs,
        out_specs=[VMEM] * len(shapes),
        scratch_shapes=list(scratch),
        compiler_params=pltpu.CompilerParams(vmem_limit_bytes=limit),
        name=name,
    )(*operands)


def terms_of(row):
    first = row.astype(bf16).astype(f32)
    second = (row - first).astype(bf16).astype(f32)
    third = (row - first - second).astype(bf16).astype(f32)
    at = lax.broadcasted_iota(jnp.int32, (SQ_ROWS, row.shape[1]), 0)
    return jnp.where(at == 0, first, jnp.where(at == 1, second, jnp.where(at == 2, third, 0.0)))


def to_lanes(column):
    square = jnp.broadcast_to(column, (column.shape[0], LANES))
    spare = jnp.zeros((LANES - column.shape[0], LANES), f32)
    return jnp.concatenate([square, spare]).T[0:1]


def to_column(row, count):
    return jnp.broadcast_to(row, (LANES, LANES)).T[:count, 0:1]


def nn(left, right):
    return jnp.dot(left, right, preferred_element_type=f32)


def nt(left, right):
    return lax.dot_general(left, right, (((1,), (1,)), ((), ())), preferred_element_type=f32)


def write_tiles(residue, own_ref, twin_ref, tiles_ref, squares_ref):
    rows = own_ref.shape[0]
    rounded = residue.astype(bf16)
    partial_value = nn(rounded[:, :rows], own_ref[...]) + nn(rounded[:, rows:], twin_ref[...])
    kept = residue.shape[0]
    squares = to_lanes(jnp.sum(residue * residue, axis=1, keepdims=True))
    squares_ref[...] = jnp.broadcast_to(squares.reshape(1, 1, LANES), squares_ref.shape)
    extra = terms_of(squares).astype(bf16)
    for j in range(tiles_ref.shape[0]):
        tiles_ref[j, :kept, :] = partial_value[:, j * LANES : (j + 1) * LANES].astype(bf16)
        tiles_ref[j, kept:, :] = extra


def masked(residue, own_count, twin_count):
    rows = residue.shape[1] // 2
    slot = lax.broadcasted_iota(jnp.int32, residue.shape, 1)
    live = (slot < own_count) | ((slot >= rows) & (slot < rows + twin_count))
    return jnp.where(live, residue, 0.0)


def start_body(own_count, twin_count, b_own, b_twin, a_own, a_twin, tiles_ref, squares_ref, residue_ref, turned):
    cols = residue_ref.shape[0]
    rows = b_own.shape[0]
    turned[:, :rows] = b_own[...].astype(f32).T
    turned[:, rows:] = b_twin[...].astype(f32).T
    mine = turned[pl.ds(pl.multiple_of(lax.axis_index("core") * cols, cols), cols), :]
    residue = masked(mine, own_count[0], twin_count[0])
    residue_ref[...] = residue
    write_tiles(residue, a_own, a_twin, tiles_ref, squares_ref)


def turn_body(first, own_count, twin_count, half_ref, sq_ref, n_ref, a_own, a_twin, old_ref, *refs):
    right_ref = None if first else refs[0]
    tiles_ref, squares_ref, residue_ref, next_ref, image_ref, norms_ref = refs[-6:]
    cols = half_ref.shape[1]
    u_norm = to_column(jnp.sqrt(sq_ref[0:1] + floor_sq), cols)
    total = jnp.concatenate([half_ref[j] for j in range(half_ref.shape[0])], axis=1)
    raw_vec = nn(total, n_ref[...]) / u_norm
    if not first:
        raw_vec = raw_vec - u_norm * right_ref[...]
    v_norm = jnp.sqrt(jnp.sum(raw_vec * raw_vec, axis=1, keepdims=True) + floor_sq)
    next_vec = raw_vec / v_norm
    next_ref[...] = next_vec
    image = nt(next_vec.astype(bf16), n_ref[...])
    image_ref[...] = image
    pushed = image.astype(bf16)
    ahead = jnp.concatenate([nt(pushed, a_own[...]), nt(pushed, a_twin[...])], axis=1)
    residue = masked(ahead - v_norm * (old_ref[...] / u_norm), own_count[0], twin_count[0])
    residue_ref[...] = residue
    norms_ref[:, :LANES] = jnp.broadcast_to(u_norm, (cols, LANES))
    norms_ref[:, LANES:] = jnp.broadcast_to(v_norm, (cols, LANES))
    write_tiles(residue, a_own, a_twin, tiles_ref, squares_ref)


def block_sum(tiles_ref, kept):
    total = jnp.sum(tiles_ref[...].astype(f32), axis=0)
    return (total[:kept], jnp.sum(total[kept:], axis=0, keepdims=True))


def plane_sum_body(tiles_ref, out_ref):
    kept = tiles_ref.shape[1] - SQ_ROWS
    rows, squares = block_sum(tiles_ref, kept)
    extra = terms_of(squares).astype(bf16)
    for j in range(out_ref.shape[0]):
        out_ref[j, :kept, :] = rows.astype(bf16)
        out_ref[j, kept:, :] = extra


def line_sum_body(tiles_ref, out_ref, sq_ref):
    rows, squares = block_sum(tiles_ref, out_ref.shape[1])
    for j in range(out_ref.shape[0]):
        out_ref[j] = rows.astype(bf16)
    sq_ref[...] = jnp.broadcast_to(squares, sq_ref.shape)


def own_place(cols, share):
    group = lax.axis_index("grp")
    per_half = cols // share
    return (group // per_half, pl.multiple_of(group % per_half * share, share))


def pack_body(*refs):
    *sources, out_ref, work = refs
    rights, images, norms = (sources[:ITERS], sources[ITERS : 2 * ITERS], sources[2 * ITERS :])
    width = rights[0].shape[1]
    start_norm = norms[0][:, 0:1]
    phi_bar, rho_bar = (start_norm, norms[0][:, LANES : LANES + 1])
    search, search_image = (rights[0][...], images[0][...])
    coeffs, solution = (jnp.zeros_like(search), jnp.zeros_like(search))
    for k in range(1, ITERS):
        u_norm, next_norm = (norms[k][:, 0:1], norms[k][:, LANES : LANES + 1])
        radius = jnp.sqrt(rho_bar * rho_bar + u_norm * u_norm)
        cosine = rho_bar / radius
        sine_part = u_norm / radius
        coupling = sine_part * next_norm
        rho_bar = -cosine * next_norm
        step = cosine * phi_bar / radius
        phi_bar = sine_part * phi_bar
        coeffs = coeffs + step * search
        solution = solution + step * search_image
        search = rights[k][...] - coupling / radius * search
        search_image = images[k][...] - coupling / radius * search_image
    for j, value in enumerate((coeffs, solution, search, search_image)):
        work[:, j * width : (j + 1) * width] = value
    for j, value in enumerate((phi_bar, rho_bar, start_norm)):
        work[:, 4 * width + j * LANES : 4 * width + (j + 1) * LANES] = jnp.broadcast_to(value, (value.shape[0], LANES))
    share = out_ref.shape[0]
    _, at = own_place(work.shape[0], share)
    out_ref[...] = work[pl.ds(at, share), :]


def final_body(everyone_ref, mine_ref, twin_ref, out_ref, coeffs_ref, ratio_ref, column):
    share = mine_ref.shape[0]
    width = out_ref.shape[1]
    tiles = everyone_ref[...].reshape(everyone_ref.shape[0], LANES)
    sender = lax.broadcasted_iota(jnp.int32, tiles.shape, 0)
    cols = column.shape[0]
    owner, at = own_place(cols, share)
    wanted = sender // lax.axis_size("grp") % 2 == owner
    squares = jnp.sum(jnp.where(wanted, tiles, 0.0), axis=0, keepdims=True)
    column[...] = jnp.broadcast_to(to_column(jnp.sqrt(squares + floor_sq), cols), column.shape)
    u_norm = column[pl.ds(at, share), :][:, 0:1]
    own = owner == lax.axis_index("core")

    def piece(start, length):
        return jnp.where(own, mine_ref[:, start : start + length], twin_ref[:, start : start + length])

    phi_bar, rho_bar, start_norm = (piece(4 * width + j * LANES, LANES)[:, 0:1] for j in range(3))
    radius = jnp.sqrt(rho_bar * rho_bar + u_norm * u_norm)
    step = rho_bar / radius * phi_bar / radius
    phi_bar = u_norm / radius * phi_bar
    coeffs_ref[...] = piece(0, width) + step * piece(2 * width, width)
    out_ref[...] = piece(width, width) + step * piece(3 * width, width)
    ratio_ref[...] = to_lanes(phi_bar / start_norm)


def exchange(tiles, axis):
    return lax.all_to_all(tiles, axis, 0, 0, tiled=True)


def swap_cores(value):
    return lax.ppermute(value, "core", [(0, 1), (1, 0)])


SMALL = 4 * 1024 * 1024


def sum_everywhere(tiles):
    peers, tall, _ = tiles.shape
    kept = tall - SQ_ROWS
    lines = lax.axis_size("grp")
    (block,) = run(plane_sum_body, [((lines, tall, LANES), bf16)], [exchange(tiles, plane)], [VMEM], "plane_sum", limit=SMALL)
    half, squares = run(
        line_sum_body,
        [((peers, kept, LANES), bf16), ((SQ_ROWS, LANES), f32)],
        [exchange(block, "grp")],
        [VMEM],
        "line_sum",
        limit=SMALL,
    )
    return (exchange(half, plane), squares)


def shards(matrix, right_side, precond, row_counts):
    local_rows, width = matrix.shape
    cols = right_side.shape[1] // 2
    twin_matrix = swap_cores(matrix)
    twin_side = swap_cores(right_side)
    twin_counts = swap_cores(row_counts)
    counts = [row_counts, twin_counts]
    blocks = [matrix, twin_matrix]
    tiles_shape = (width // LANES, cols + SQ_ROWS, LANES)
    tiles, _, residue = run(
        start_body,
        [(tiles_shape, bf16), ((1, 1, LANES), f32), ((cols, 2 * local_rows), f32)],
        [*counts, right_side, twin_side, *blocks],
        [SMEM] * 2 + [VMEM] * 4,
        "start",
        scratch=[pltpu.VMEM((2 * cols, 2 * local_rows), f32)],
        limit=12 * 1024 * 1024,
    )

    def turn(first, half, squares, right_vec, residue, copies=1):
        return run(
            functools.partial(turn_body, first),
            [
                (tiles_shape, bf16),
                ((copies, 1, LANES), f32),
                (residue.shape, f32),
                ((cols, width), f32),
                ((cols, width), f32),
                ((cols, 2 * LANES), f32),
            ],
            [*counts, half, squares, precond, *blocks, residue] + ([] if first else [right_vec]),
            [SMEM] * 2 + [VMEM] * (6 if first else 7),
            "turn",
            limit=20 * 1024 * 1024,
        )

    right_vec = None
    rights, images, norms = ([], [], [])
    for turn_index in range(ITERS):
        half, squares = sum_everywhere(tiles)
        tiles, local_squares, residue, right_vec, image, norm_pair = turn(
            turn_index == 0,
            half,
            squares,
            right_vec,
            residue,
            lax.axis_size(every) if turn_index + 1 == ITERS else 1,
        )
        rights.append(right_vec)
        images.append(image)
        norms.append(norm_pair)
    half, squares = sum_everywhere(tiles)
    turn(False, half, squares, right_vec, residue)
    everyone = exchange(local_squares, every)

    share = 2 * cols // lax.axis_size("grp")
    packed = run(
        pack_body,
        [((share, 4 * width + 3 * LANES), f32)],
        [*rights, *images, *norms],
        [VMEM] * (3 * ITERS),
        "pack",
        scratch=[pltpu.VMEM((cols, 4 * width + 3 * LANES), f32)],
        limit=12 * 1024 * 1024,
    )[0]
    twin_packed = swap_cores(packed)
    out, coeffs, ratio = run(
        final_body,
        [((share, width), f32), ((share, width), f32), ((1, LANES), f32)],
        [everyone, packed, twin_packed],
        [VMEM] * 3,
        "final",
        scratch=[pltpu.VMEM((cols, LANES), f32)],
        limit=12 * 1024 * 1024,
    )
    return (out.T, coeffs.T, ratio[0, :share])


def solution(mesh):
    fine = Mesh(mesh.devices.reshape(4, 4, 2, 8), every)
    return jax.shard_map(
        shards,
        mesh=fine,
        in_specs=(P(every, None), P(every, None), P(), P(every)),
        out_specs=(P(None, "grp"), P(None, "grp"), P("grp")),
        check_vma=False,
    )
```

```python
import functools

import jax
import jax.numpy as jnp
from jax import lax
from jax.experimental import pallas as pl
from jax.experimental.pallas import tpu as pltpu
from jax.sharding import Mesh, PartitionSpec as P

ITERS = 3

floor_sq = 0.01
plane = ("y", "x")
every = ("y", "x", "core", "grp")
SQ_ROWS = 8
LANES = 128
LOAD_ROWS = 256
bf16, f32 = jnp.bfloat16, jnp.float32
VMEM = pl.BlockSpec(memory_space=pltpu.VMEM)
SMEM = pl.BlockSpec(memory_space=pltpu.SMEM)


def run(body, shapes, operands, specs, name, scratch=(), limit=None):
    return pl.pallas_call(
        body,
        out_shape=[jax.ShapeDtypeStruct(s, t) for s, t in shapes],
        in_specs=specs,
        out_specs=[VMEM] * len(shapes),
        scratch_shapes=list(scratch),
        compiler_params=pltpu.CompilerParams(vmem_limit_bytes=limit),
        name=name,
    )(*operands)


def terms_of(row):
    first = row.astype(bf16).astype(f32)
    second = (row - first).astype(bf16).astype(f32)
    third = (row - first - second).astype(bf16).astype(f32)
    at = lax.broadcasted_iota(jnp.int32, (SQ_ROWS, row.shape[1]), 0)
    return jnp.where(at == 0, first, jnp.where(at == 1, second, jnp.where(at == 2, third, 0.0)))


def to_lanes(column):
    square = jnp.broadcast_to(column, (column.shape[0], LANES))
    spare = jnp.zeros((LANES - column.shape[0], LANES), f32)
    return jnp.concatenate([square, spare]).T[0:1]


def to_column(row, count):
    return jnp.broadcast_to(row, (LANES, LANES)).T[:count, 0:1]


def nn(left, right):
    return jnp.dot(left, right, preferred_element_type=f32)


def nt(left, right):
    return lax.dot_general(left, right, (((1,), (1,)), ((), ())), preferred_element_type=f32)


def write_tiles(residue, own_ref, twin_ref, tiles_ref, squares_ref):
    rows = own_ref.shape[0]
    rounded = residue.astype(bf16)
    partial_value = nn(rounded[:, :rows], own_ref[...]) + nn(rounded[:, rows:], twin_ref[...])
    kept = residue.shape[0]
    squares = to_lanes(jnp.sum(residue * residue, axis=1, keepdims=True))
    squares_ref[...] = jnp.broadcast_to(squares.reshape(1, 1, LANES), squares_ref.shape)
    extra = terms_of(squares).astype(bf16)
    for j in range(tiles_ref.shape[0]):
        tiles_ref[j, :kept, :] = partial_value[:, j * LANES : (j + 1) * LANES].astype(bf16)
        tiles_ref[j, kept:, :] = extra


def masked(residue, own_count, twin_count):
    rows = residue.shape[1] // 2
    slot = lax.broadcasted_iota(jnp.int32, residue.shape, 1)
    live = (slot < own_count) | ((slot >= rows) & (slot < rows + twin_count))
    return jnp.where(live, residue, 0.0)


def load_body(n_in, a_in, n_ref, turned_n, a_ref, turned_a, arrived):
    jobs = []
    for source, target, turned in ((a_in, a_ref, turned_a), (n_in, n_ref, turned_n)):
        for at in range(0, source.shape[0], LOAD_ROWS):
            block = pl.ds(at, LOAD_ROWS)
            copy = pltpu.make_async_copy(source.at[block], target.at[block], arrived.at[len(jobs)])
            copy.start()
            jobs.append((copy, target, turned, at))
    for copy, target, turned, at in jobs:
        copy.wait()
        turned[:, at : at + LOAD_ROWS] = target[at : at + LOAD_ROWS, :].T


def start_body(own_count, twin_count, b_own, b_twin, a_own, a_twin, tiles_ref, squares_ref, residue_ref, turned):
    cols = residue_ref.shape[0]
    rows = b_own.shape[0]
    turned[:, :rows] = b_own[...].astype(f32).T
    turned[:, rows:] = b_twin[...].astype(f32).T
    mine = turned[pl.ds(pl.multiple_of(lax.axis_index("core") * cols, cols), cols), :]
    residue = masked(mine, own_count[0], twin_count[0])
    residue_ref[...] = residue
    write_tiles(residue, a_own, a_twin, tiles_ref, squares_ref)


def turn_body(first, own_count, twin_count, half_ref, sq_ref, n_ref, turned_n, a_own, a_twin, turned_a, old_ref, *refs):
    right_ref = None if first else refs[0]
    tiles_ref, squares_ref, residue_ref, next_ref, image_ref, norms_ref = refs[-6:]
    cols = half_ref.shape[1]
    u_norm = to_column(jnp.sqrt(sq_ref[0:1] + floor_sq), cols)
    total = jnp.concatenate([half_ref[j] for j in range(half_ref.shape[0])], axis=1)
    raw_vec = nn(total, n_ref[...]) / u_norm
    if not first:
        raw_vec = raw_vec - u_norm * right_ref[...]
    v_norm = jnp.sqrt(jnp.sum(raw_vec * raw_vec, axis=1, keepdims=True) + floor_sq)
    next_vec = raw_vec / v_norm
    next_ref[...] = next_vec
    image = nn(next_vec.astype(bf16), turned_n[...])
    image_ref[...] = image
    pushed = image.astype(bf16)
    ahead = jnp.concatenate([nn(pushed, turned_a[...]), nt(pushed, a_twin[...])], axis=1)
    residue = masked(ahead - v_norm * (old_ref[...] / u_norm), own_count[0], twin_count[0])
    residue_ref[...] = residue
    norms_ref[:, :LANES] = jnp.broadcast_to(u_norm, (cols, LANES))
    norms_ref[:, LANES:] = jnp.broadcast_to(v_norm, (cols, LANES))
    write_tiles(residue, a_own, a_twin, tiles_ref, squares_ref)


def block_sum(tiles_ref, kept):
    total = jnp.sum(tiles_ref[...].astype(f32), axis=0)
    return (total[:kept], jnp.sum(total[kept:], axis=0, keepdims=True))


def plane_sum_body(tiles_ref, out_ref):
    kept = tiles_ref.shape[1] - SQ_ROWS
    rows, squares = block_sum(tiles_ref, kept)
    extra = terms_of(squares).astype(bf16)
    for j in range(out_ref.shape[0]):
        out_ref[j, :kept, :] = rows.astype(bf16)
        out_ref[j, kept:, :] = extra


def line_sum_body(tiles_ref, out_ref, sq_ref):
    rows, squares = block_sum(tiles_ref, out_ref.shape[1])
    for j in range(out_ref.shape[0]):
        out_ref[j] = rows.astype(bf16)
    sq_ref[...] = jnp.broadcast_to(squares, sq_ref.shape)


def own_place(cols, share):
    group = lax.axis_index("grp")
    per_half = cols // share
    return (group // per_half, pl.multiple_of(group % per_half * share, share))


def pack_body(*refs):
    *sources, out_ref = refs
    share = out_ref.shape[0]
    _, at = own_place(sources[0].shape[0], share)
    sources = [ref.at[pl.ds(at, share)] for ref in sources]
    rights, images, norms = (sources[:ITERS], sources[ITERS : 2 * ITERS], sources[2 * ITERS :])
    width = rights[0].shape[1]
    start_norm = norms[0][:, 0:1]
    phi_bar, rho_bar = (start_norm, norms[0][:, LANES : LANES + 1])
    search, search_image = (rights[0][...], images[0][...])
    coeffs, solution = (jnp.zeros_like(search), jnp.zeros_like(search))
    for k in range(1, ITERS):
        u_norm, next_norm = (norms[k][:, 0:1], norms[k][:, LANES : LANES + 1])
        radius = jnp.sqrt(rho_bar * rho_bar + u_norm * u_norm)
        cosine = rho_bar / radius
        sine_part = u_norm / radius
        coupling = sine_part * next_norm
        rho_bar = -cosine * next_norm
        step = cosine * phi_bar / radius
        phi_bar = sine_part * phi_bar
        coeffs = coeffs + step * search
        solution = solution + step * search_image
        search = rights[k][...] - coupling / radius * search
        search_image = images[k][...] - coupling / radius * search_image
    for j, value in enumerate((coeffs, solution, search, search_image)):
        out_ref[:, j * width : (j + 1) * width] = value
    for j, value in enumerate((phi_bar, rho_bar, start_norm)):
        out_ref[:, 4 * width + j * LANES : 4 * width + (j + 1) * LANES] = jnp.broadcast_to(value, (share, LANES))


def final_body(everyone_ref, mine_ref, twin_ref, out_ref, coeffs_ref, ratio_ref, column):
    share = mine_ref.shape[0]
    width = out_ref.shape[1]
    tiles = everyone_ref[...].reshape(everyone_ref.shape[0], LANES)
    sender = lax.broadcasted_iota(jnp.int32, tiles.shape, 0)
    cols = column.shape[0]
    owner, at = own_place(cols, share)
    wanted = sender // lax.axis_size("grp") % 2 == owner
    squares = jnp.sum(jnp.where(wanted, tiles, 0.0), axis=0, keepdims=True)
    column[...] = jnp.broadcast_to(to_column(jnp.sqrt(squares + floor_sq), cols), column.shape)
    u_norm = column[pl.ds(at, share), :][:, 0:1]
    own = owner == lax.axis_index("core")

    def piece(start, length):
        return jnp.where(own, mine_ref[:, start : start + length], twin_ref[:, start : start + length])

    phi_bar, rho_bar, start_norm = (piece(4 * width + j * LANES, LANES)[:, 0:1] for j in range(3))
    radius = jnp.sqrt(rho_bar * rho_bar + u_norm * u_norm)
    step = rho_bar / radius * phi_bar / radius
    phi_bar = u_norm / radius * phi_bar
    coeffs_ref[...] = piece(0, width) + step * piece(2 * width, width)
    out_ref[...] = piece(width, width) + step * piece(3 * width, width)
    ratio_ref[...] = to_lanes(phi_bar / start_norm)[:, :share]


def exchange(tiles, axis):
    return lax.all_to_all(tiles, axis, 0, 0, tiled=True)


def swap_cores(value):
    return lax.ppermute(value, "core", [(0, 1), (1, 0)])


SMALL = 4 * 1024 * 1024


def sum_everywhere(tiles):
    peers, tall, _ = tiles.shape
    kept = tall - SQ_ROWS
    lines = lax.axis_size("grp")
    (block,) = run(plane_sum_body, [((lines, tall, LANES), bf16)], [exchange(tiles, plane)], [VMEM], "plane_sum", limit=SMALL)
    half, squares = run(
        line_sum_body,
        [((peers, kept, LANES), bf16), ((SQ_ROWS, LANES), f32)],
        [exchange(block, "grp")],
        [VMEM],
        "line_sum",
        limit=SMALL,
    )
    return (exchange(half, plane), squares)


def shards(matrix, right_side, precond, row_counts):
    local_rows, width = matrix.shape
    cols = right_side.shape[1] // 2
    twin_matrix = swap_cores(matrix)
    twin_side = swap_cores(right_side)
    twin_counts = swap_cores(row_counts)
    counts = [row_counts, twin_counts]
    anywhere = pl.BlockSpec(memory_space=pltpu.HBM)
    held, turned, own, turned_own = run(
        load_body,
        [(precond.shape, bf16), (precond.shape[::-1], bf16), (matrix.shape, bf16), (matrix.shape[::-1], bf16)],
        [precond, matrix],
        [anywhere] * 2,
        "load",
        scratch=[pltpu.SemaphoreType.DMA(((width + local_rows) // LOAD_ROWS,))],
        limit=24 * 1024 * 1024,
    )
    blocks = [own, twin_matrix]
    tiles_shape = (width // LANES, cols + SQ_ROWS, LANES)
    tiles, _, residue = run(
        start_body,
        [(tiles_shape, bf16), ((1, 1, LANES), f32), ((cols, 2 * local_rows), f32)],
        [*counts, right_side, twin_side, *blocks],
        [SMEM] * 2 + [VMEM] * 4,
        "start",
        scratch=[pltpu.VMEM((2 * cols, 2 * local_rows), f32)],
        limit=12 * 1024 * 1024,
    )

    def turn(first, half, squares, right_vec, residue, copies=1):
        return run(
            functools.partial(turn_body, first),
            [
                (tiles_shape, bf16),
                ((copies, 1, LANES), f32),
                (residue.shape, f32),
                ((cols, width), f32),
                ((cols, width), f32),
                ((cols, 2 * LANES), f32),
            ],
            [*counts, half, squares, held, turned, *blocks, turned_own, residue] + ([] if first else [right_vec]),
            [SMEM] * 2 + [VMEM] * (8 if first else 9),
            "turn",
            limit=20 * 1024 * 1024,
        )

    right_vec = None
    rights, images, norms = ([], [], [])
    for turn_index in range(ITERS):
        half, squares = sum_everywhere(tiles)
        tiles, local_squares, residue, right_vec, image, norm_pair = turn(
            turn_index == 0,
            half,
            squares,
            right_vec,
            residue,
            lax.axis_size(every) if turn_index + 1 == ITERS else 1,
        )
        rights.append(right_vec)
        images.append(image)
        norms.append(norm_pair)
    half, squares = sum_everywhere(tiles)
    turn(False, half, squares, right_vec, residue)
    everyone = exchange(local_squares, every)

    share = 2 * cols // lax.axis_size("grp")
    packed = run(
        pack_body,
        [((share, 4 * width + 3 * LANES), f32)],
        [*rights, *images, *norms],
        [VMEM] * (3 * ITERS),
        "pack",
        limit=12 * 1024 * 1024,
    )[0]
    twin_packed = swap_cores(packed)
    out, coeffs, ratio = run(
        final_body,
        [((share, width), f32), ((share, width), f32), ((1, share), f32)],
        [everyone, packed, twin_packed],
        [VMEM] * 3,
        "final",
        scratch=[pltpu.VMEM((cols, LANES), f32)],
        limit=12 * 1024 * 1024,
    )
    return (out.T, coeffs.T, ratio[0])


def solution(mesh):
    fine = Mesh(mesh.devices.reshape(4, 4, 2, 8), every)
    return jax.shard_map(
        shards,
        mesh=fine,
        in_specs=(P(every, None), P(every, None), P(), P(every)),
        out_specs=(P(None, "grp"), P(None, "grp"), P("grp")),
        check_vma=False,
    )
```

```python
import functools

import jax
import jax.numpy as jnp
from jax import lax
from jax.experimental import pallas as pl
from jax.experimental.pallas import tpu as pltpu
from jax.sharding import Mesh, PartitionSpec as P

ITERS = 3

floor_sq = 0.01
plane = ("y", "x")
every = ("y", "x", "core", "grp")
SQ_ROWS = 8
LANES = 128
LOAD_ROWS = 256
bf16, f32 = jnp.bfloat16, jnp.float32
VMEM = pl.BlockSpec(memory_space=pltpu.VMEM)
SMEM = pl.BlockSpec(memory_space=pltpu.SMEM)


def run(body, shapes, operands, specs, name, scratch=(), limit=None):
    return pl.pallas_call(
        body,
        out_shape=[jax.ShapeDtypeStruct(s, t) for s, t in shapes],
        in_specs=specs,
        out_specs=[VMEM] * len(shapes),
        scratch_shapes=list(scratch),
        compiler_params=pltpu.CompilerParams(vmem_limit_bytes=limit),
        name=name,
    )(*operands)


def terms_of(row):
    first = row.astype(bf16).astype(f32)
    second = (row - first).astype(bf16).astype(f32)
    third = (row - first - second).astype(bf16).astype(f32)
    at = lax.broadcasted_iota(jnp.int32, (SQ_ROWS, row.shape[1]), 0)
    return jnp.where(at == 0, first, jnp.where(at == 1, second, jnp.where(at == 2, third, 0.0)))


def to_lanes(column):
    square = jnp.broadcast_to(column, (column.shape[0], LANES))
    spare = jnp.zeros((LANES - column.shape[0], LANES), f32)
    return jnp.concatenate([square, spare]).T[0:1]


def to_column(row, count):
    return jnp.broadcast_to(row, (LANES, LANES)).T[:count, 0:1]


def nn(left, right):
    return jnp.dot(left, right, preferred_element_type=f32)


def squares_of(residue):
    return to_lanes(jnp.sum(residue * residue, axis=1, keepdims=True))


def put_tiles(partial_value, squares, tiles_ref):
    kept = partial_value.shape[0]
    extra = terms_of(squares).astype(bf16)
    for j in range(tiles_ref.shape[0]):
        tiles_ref[j, :kept, :] = partial_value[:, j * LANES : (j + 1) * LANES].astype(bf16)
        tiles_ref[j, kept:, :] = extra


def write_tiles(residue, own_ref, twin_ref, tiles_ref):
    rows = own_ref.shape[0]
    rounded = residue.astype(bf16)
    partial_value = nn(rounded[:, :rows], own_ref[...]) + nn(rounded[:, rows:], twin_ref[...])
    put_tiles(partial_value, squares_of(residue), tiles_ref)


def tiles_body(residue_ref, own_ref, twin_ref, tiles_ref):
    write_tiles(residue_ref[...], own_ref, twin_ref, tiles_ref)


def masked(residue, own_count, twin_count):
    rows = residue.shape[1] // 2
    slot = lax.broadcasted_iota(jnp.int32, residue.shape, 1)
    live = (slot < own_count) | ((slot >= rows) & (slot < rows + twin_count))
    return jnp.where(live, residue, 0.0)


def load_body(source, held, turned, arrived):
    copies = []
    for at in range(0, source.shape[0], LOAD_ROWS):
        block = pl.ds(at, LOAD_ROWS)
        copy = pltpu.make_async_copy(source.at[block], held.at[block], arrived.at[len(copies)])
        copy.start()
        copies.append((copy, at))
    for copy, at in copies:
        copy.wait()
        turned[:, at : at + LOAD_ROWS] = held[at : at + LOAD_ROWS, :].T


def start_body(own_count, twin_count, b_own, b_twin, a_own, a_twin, tiles_ref, residue_ref, turned_own, turned_twin, work):
    cols = residue_ref.shape[0]
    rows = b_own.shape[0]
    work[:, :rows] = b_own[...].astype(f32).T
    work[:, rows:] = b_twin[...].astype(f32).T
    mine = work[pl.ds(pl.multiple_of(lax.axis_index("core") * cols, cols), cols), :]
    residue = masked(mine, own_count[0], twin_count[0])
    residue_ref[...] = residue
    turned_own[...] = a_own[...].T
    turned_twin[...] = a_twin[...].T
    write_tiles(residue, a_own, a_twin, tiles_ref)


def turn_body(first, last, own_count, twin_count, half_ref, sq_ref, n_ref, turned_n, a_own, a_twin, turned_own, turned_twin, old_ref, *refs):
    right_ref = None if first else refs[0]
    sent_ref, residue_ref, next_ref, image_ref, norms_ref = refs[-5:]
    cols = half_ref.shape[1]
    u_norm = to_column(jnp.sqrt(sq_ref[0:1] + floor_sq), cols)
    per_u = 1.0 / u_norm
    total = jnp.concatenate([half_ref[j] for j in range(half_ref.shape[0])], axis=1)
    raw_vec = nn(total, n_ref[...]) * per_u
    if not first:
        raw_vec = raw_vec - u_norm * right_ref[...]
    image = nn(raw_vec.astype(bf16), turned_n[...])
    v_norm = jnp.sqrt(jnp.sum(raw_vec * raw_vec, axis=1, keepdims=True) + floor_sq)
    per_v = 1.0 / v_norm
    next_ref[...] = raw_vec * per_v
    image = image * per_v
    image_ref[...] = image
    pushed = image.astype(bf16)
    ahead = jnp.concatenate([nn(pushed, turned_own[...]), nn(pushed, turned_twin[...])], axis=1)
    residue = masked(ahead - (v_norm * per_u) * old_ref[...], own_count[0], twin_count[0])
    residue_ref[...] = residue
    norms_ref[:, :LANES] = jnp.broadcast_to(u_norm, (cols, LANES))
    norms_ref[:, LANES:] = jnp.broadcast_to(v_norm, (cols, LANES))
    if last:
        sent_ref[...] = jnp.broadcast_to(squares_of(residue).reshape(1, 1, LANES), sent_ref.shape)
    else:
        write_tiles(residue, a_own, a_twin, sent_ref)


def block_sum(tiles_ref, kept):
    total = jnp.sum(tiles_ref[...].astype(f32), axis=0)
    return (total[:kept], jnp.sum(total[kept:], axis=0, keepdims=True))


def plane_sum_body(tiles_ref, out_ref):
    kept = tiles_ref.shape[1] - SQ_ROWS
    rows, squares = block_sum(tiles_ref, kept)
    extra = terms_of(squares).astype(bf16)
    for j in range(out_ref.shape[0]):
        out_ref[j, :kept, :] = rows.astype(bf16)
        out_ref[j, kept:, :] = extra


def line_sum_body(tiles_ref, out_ref, sq_ref):
    rows, squares = block_sum(tiles_ref, out_ref.shape[1])
    for j in range(out_ref.shape[0]):
        out_ref[j] = rows.astype(bf16)
    sq_ref[...] = jnp.broadcast_to(squares, sq_ref.shape)


def own_place(cols, share):
    group = lax.axis_index("grp")
    per_half = cols // share
    return (group // per_half, pl.multiple_of(group % per_half * share, share))


def pack_body(*refs):
    *sources, out_ref = refs
    share = out_ref.shape[0]
    _, at = own_place(sources[0].shape[0], share)
    sources = [ref.at[pl.ds(at, share)] for ref in sources]
    rights, images, norms = (sources[:ITERS], sources[ITERS : 2 * ITERS], sources[2 * ITERS :])
    width = rights[0].shape[1]
    start_norm = norms[0][:, 0:1]
    phi_bar, rho_bar = (start_norm, norms[0][:, LANES : LANES + 1])
    search, search_image = (rights[0][...], images[0][...])
    coeffs, solution = (jnp.zeros_like(search), jnp.zeros_like(search))
    for k in range(1, ITERS):
        u_norm, next_norm = (norms[k][:, 0:1], norms[k][:, LANES : LANES + 1])
        radius = jnp.sqrt(rho_bar * rho_bar + u_norm * u_norm)
        cosine = rho_bar / radius
        sine_part = u_norm / radius
        coupling = sine_part * next_norm
        rho_bar = -cosine * next_norm
        step = cosine * phi_bar / radius
        phi_bar = sine_part * phi_bar
        coeffs = coeffs + step * search
        solution = solution + step * search_image
        search = rights[k][...] - coupling / radius * search
        search_image = images[k][...] - coupling / radius * search_image
    for j, value in enumerate((coeffs, solution, search, search_image)):
        out_ref[:, j * width : (j + 1) * width] = value
    for j, value in enumerate((phi_bar, rho_bar, start_norm)):
        out_ref[:, 4 * width + j * LANES : 4 * width + (j + 1) * LANES] = jnp.broadcast_to(value, (share, LANES))


def final_body(everyone_ref, mine_ref, twin_ref, out_ref, coeffs_ref, ratio_ref, column):
    share = mine_ref.shape[0]
    width = out_ref.shape[1]
    cols = column.shape[0]
    owner, at = own_place(cols, share)
    lines = lax.axis_size("grp")
    by_core = [jnp.zeros((1, LANES), f32), jnp.zeros((1, LANES), f32)]
    for sender in range(0, everyone_ref.shape[0], lines):
        half = sender // lines % 2
        by_core[half] = by_core[half] + jnp.sum(everyone_ref[sender : sender + lines], axis=0)
    squares = jnp.where(owner == 0, by_core[0], by_core[1])
    column[...] = jnp.broadcast_to(to_column(jnp.sqrt(squares + floor_sq), cols), column.shape)
    u_norm = column[pl.ds(at, share), :][:, 0:1]
    own = owner == lax.axis_index("core")

    def piece(start, length):
        return jnp.where(own, mine_ref[:, start : start + length], twin_ref[:, start : start + length])

    phi_bar, rho_bar, start_norm = (piece(4 * width + j * LANES, LANES)[:, 0:1] for j in range(3))
    radius = jnp.sqrt(rho_bar * rho_bar + u_norm * u_norm)
    step = rho_bar / radius * phi_bar / radius
    phi_bar = u_norm / radius * phi_bar
    coeffs_ref[...] = piece(0, width) + step * piece(2 * width, width)
    out_ref[...] = piece(width, width) + step * piece(3 * width, width)
    ratio_ref[...] = to_lanes(phi_bar / start_norm)[:, :share]


def exchange(tiles, axis):
    return lax.all_to_all(tiles, axis, 0, 0, tiled=True)


def swap_cores(value):
    return lax.ppermute(value, "core", [(0, 1), (1, 0)])


SMALL = 4 * 1024 * 1024


def sum_everywhere(tiles):
    peers, tall, _ = tiles.shape
    kept = tall - SQ_ROWS
    lines = lax.axis_size("grp")
    (block,) = run(plane_sum_body, [((lines, tall, LANES), bf16)], [exchange(tiles, plane)], [VMEM], "plane_sum", limit=SMALL)
    half, squares = run(
        line_sum_body,
        [((peers, kept, LANES), bf16), ((SQ_ROWS, LANES), f32)],
        [exchange(block, "grp")],
        [VMEM],
        "line_sum",
        limit=SMALL,
    )
    return (exchange(half, plane), squares)


def shards(matrix, right_side, precond, row_counts):
    local_rows, width = matrix.shape
    cols = right_side.shape[1] // 2
    tiles_shape = (width // LANES, cols + SQ_ROWS, LANES)
    twin_matrix, twin_side, twin_counts = (swap_cores(value) for value in (matrix, right_side, row_counts))
    counts = [row_counts, twin_counts]
    blocks = [matrix, twin_matrix]
    held, turned = run(
        load_body,
        [(precond.shape, bf16), (precond.shape[::-1], bf16)],
        [precond],
        [pl.BlockSpec(memory_space=pltpu.HBM)],
        "load",
        scratch=[pltpu.SemaphoreType.DMA((width // LOAD_ROWS,))],
        limit=36 * 1024 * 1024,
    )
    right_side, turned = lax.optimization_barrier((right_side, turned))
    tiles, residue, turned_own, turned_twin = run(
        start_body,
        [
            (tiles_shape, bf16),
            ((cols, 2 * local_rows), f32),
            (matrix.shape[::-1], bf16),
            (matrix.shape[::-1], bf16),
        ],
        [*counts, right_side, twin_side, *blocks],
        [SMEM] * 2 + [VMEM] * 4,
        "start",
        scratch=[pltpu.VMEM((2 * cols, 2 * local_rows), f32)],
        limit=12 * 1024 * 1024,
    )

    def turn(half, squares, right_vec, residue, last=False):
        first = right_vec is None
        sent = ((lax.axis_size(every), 1, LANES), f32) if last else (tiles_shape, bf16)
        return run(
            functools.partial(turn_body, first, last),
            [sent, (residue.shape, f32), ((cols, width), f32), ((cols, width), f32), ((cols, 2 * LANES), f32)],
            [*counts, half, squares, held, turned, *blocks, turned_own, turned_twin, residue] + ([] if first else [right_vec]),
            [SMEM] * 2 + [VMEM] * (9 if first else 10),
            "turn",
            limit=20 * 1024 * 1024,
        )

    right_vec = None
    rights, images, norms = ([], [], [])
    for turn_index in range(ITERS):
        last = turn_index + 1 == ITERS
        half, squares = sum_everywhere(tiles)
        tiles, residue, right_vec, image, norm_pair = turn(half, squares, right_vec, residue, last)
        rights.append(right_vec)
        images.append(image)
        norms.append(norm_pair)
    everyone = exchange(tiles, every)
    (tiles,) = run(tiles_body, [(tiles_shape, bf16)], [residue, *blocks], [VMEM] * 3, "tiles", limit=20 * 1024 * 1024)
    half, squares = sum_everywhere(tiles)
    turn(half, squares, right_vec, residue)

    share = 2 * cols // lax.axis_size("grp")
    packed = run(
        pack_body,
        [((share, 4 * width + 3 * LANES), f32)],
        [*rights, *images, *norms],
        [VMEM] * (3 * ITERS),
        "pack",
        limit=12 * 1024 * 1024,
    )[0]
    twin_packed = swap_cores(packed)
    out, coeffs, ratio = run(
        final_body,
        [((share, width), f32), ((share, width), f32), ((1, share), f32)],
        [everyone, packed, twin_packed],
        [VMEM] * 3,
        "final",
        scratch=[pltpu.VMEM((cols, LANES), f32)],
        limit=12 * 1024 * 1024,
    )
    return (out.T, coeffs.T, ratio[0])


def solution(mesh):
    fine = Mesh(mesh.devices.reshape(4, 4, 2, 8), every)
    return jax.shard_map(
        shards,
        mesh=fine,
        in_specs=(P(every, None), P(every, None), P(), P(every)),
        out_specs=(P(None, "grp"), P(None, "grp"), P("grp")),
        check_vma=False,
    )
```

```python
import functools
import itertools

import jax
import jax.numpy as jnp
from jax import lax
from jax.experimental import pallas as pl
from jax.experimental.pallas import tpu as pltpu
from jax.sharding import Mesh, PartitionSpec as P

ITERS = 3

floor_sq = 0.01
every = ("y", "x", "core", "grp")
SQ_ROWS = 8
LANES = 128
LOAD_ROWS = 256
bf16, f32 = jnp.bfloat16, jnp.float32
VMEM = pl.BlockSpec(memory_space=pltpu.VMEM)
SMEM = pl.BlockSpec(memory_space=pltpu.SMEM)


def run(body, shapes, operands, specs, name, scratch=(), limit=None):
    return pl.pallas_call(
        body,
        out_shape=[jax.ShapeDtypeStruct(s, t) for s, t in shapes],
        in_specs=specs,
        out_specs=[VMEM] * len(shapes),
        scratch_shapes=list(scratch),
        compiler_params=pltpu.CompilerParams(vmem_limit_bytes=limit),
        name=name,
    )(*operands)


def terms_of(row):
    first = row.astype(bf16).astype(f32)
    second = (row - first).astype(bf16).astype(f32)
    third = (row - first - second).astype(bf16).astype(f32)
    at = lax.broadcasted_iota(jnp.int32, (SQ_ROWS, row.shape[1]), 0)
    return jnp.where(at == 0, first, jnp.where(at == 1, second, jnp.where(at == 2, third, 0.0)))


def to_lanes(column):
    square = jnp.broadcast_to(column, (column.shape[0], LANES))
    spare = jnp.zeros((LANES - column.shape[0], LANES), f32)
    return jnp.concatenate([square, spare]).T[0:1]


def to_column(row, count):
    return jnp.broadcast_to(row, (LANES, LANES)).T[:count, 0:1]


def nn(left, right):
    return jnp.dot(left, right, preferred_element_type=f32)


def squares_of(residue):
    return to_lanes(jnp.sum(residue * residue, axis=1, keepdims=True))


def put_tiles(partial_value, squares, tiles_ref):
    kept = partial_value.shape[0]
    extra = terms_of(squares).astype(bf16)
    for j in range(tiles_ref.shape[0]):
        tiles_ref[j, :kept, :] = partial_value[:, j * LANES : (j + 1) * LANES].astype(bf16)
        tiles_ref[j, kept:, :] = extra


def write_tiles(residue, own_ref, twin_ref, tiles_ref):
    rows = own_ref.shape[0]
    rounded = residue.astype(bf16)
    partial_value = nn(rounded[:, :rows], own_ref[...]) + nn(rounded[:, rows:], twin_ref[...])
    put_tiles(partial_value, squares_of(residue), tiles_ref)


def tiles_body(residue_ref, own_ref, twin_ref, tiles_ref):
    write_tiles(residue_ref[...], own_ref, twin_ref, tiles_ref)


def masked(residue, own_count, twin_count):
    rows = residue.shape[1] // 2
    slot = lax.broadcasted_iota(jnp.int32, residue.shape, 1)
    live = (slot < own_count) | ((slot >= rows) & (slot < rows + twin_count))
    return jnp.where(live, residue, 0.0)


def load_body(source, held, turned, arrived):
    copies = []
    for at in range(0, source.shape[0], LOAD_ROWS):
        block = pl.ds(at, LOAD_ROWS)
        copy = pltpu.make_async_copy(source.at[block], held.at[block], arrived.at[len(copies)])
        copy.start()
        copies.append((copy, at))
    for copy, at in copies:
        copy.wait()
        turned[:, at : at + LOAD_ROWS] = held[at : at + LOAD_ROWS, :].T


def start_body(own_count, twin_count, b_own, b_twin, a_own, a_twin, tiles_ref, residue_ref, turned_own, turned_twin, work):
    cols = residue_ref.shape[0]
    rows = b_own.shape[0]
    work[:, :rows] = b_own[...].astype(f32).T
    work[:, rows:] = b_twin[...].astype(f32).T
    mine = work[pl.ds(pl.multiple_of(own_half() * cols, cols), cols), :]
    residue = masked(mine, own_count[0], twin_count[0])
    residue_ref[...] = residue
    turned_own[...] = a_own[...].T
    turned_twin[...] = a_twin[...].T
    write_tiles(residue, a_own, a_twin, tiles_ref)


def turn_body(first, last, own_count, twin_count, half_ref, sq_ref, n_ref, turned_n, a_own, a_twin, turned_own, turned_twin, old_ref, *refs):
    right_ref = None if first else refs[0]
    sent_ref, residue_ref, next_ref, image_ref, norms_ref = refs[-5:]
    cols = half_ref.shape[1]
    u_norm = to_column(jnp.sqrt(sq_ref[0:1] + floor_sq), cols)
    per_u = 1.0 / u_norm
    total = jnp.concatenate([half_ref[j] for j in range(half_ref.shape[0])], axis=1)
    raw_vec = nn(total, n_ref[...]) * per_u
    if not first:
        raw_vec = raw_vec - u_norm * right_ref[...]
    image = nn(raw_vec.astype(bf16), turned_n[...])
    v_norm = jnp.sqrt(jnp.sum(raw_vec * raw_vec, axis=1, keepdims=True) + floor_sq)
    per_v = 1.0 / v_norm
    next_ref[...] = raw_vec * per_v
    image = image * per_v
    image_ref[...] = image
    pushed = image.astype(bf16)
    ahead = jnp.concatenate([nn(pushed, turned_own[...]), nn(pushed, turned_twin[...])], axis=1)
    residue = masked(ahead - (v_norm * per_u) * old_ref[...], own_count[0], twin_count[0])
    residue_ref[...] = residue
    norms_ref[:, :LANES] = jnp.broadcast_to(u_norm, (cols, LANES))
    norms_ref[:, LANES:] = jnp.broadcast_to(v_norm, (cols, LANES))
    if last:
        sent_ref[...] = jnp.broadcast_to(squares_of(residue).reshape(1, 1, LANES), sent_ref.shape)
    else:
        write_tiles(residue, a_own, a_twin, sent_ref)


def block_sum(tiles_ref, kept):
    total = jnp.sum(tiles_ref[...].astype(f32), axis=0)
    return (total[:kept], jnp.sum(total[kept:], axis=0, keepdims=True))


def plane_sum_body(tiles_ref, out_ref):
    kept = tiles_ref.shape[1] - SQ_ROWS
    rows, squares = block_sum(tiles_ref, kept)
    extra = terms_of(squares).astype(bf16)
    for j in range(out_ref.shape[0]):
        out_ref[j, :kept, :] = rows.astype(bf16)
        out_ref[j, kept:, :] = extra


def line_sum_body(tiles_ref, out_ref, sq_ref):
    rows, squares = block_sum(tiles_ref, out_ref.shape[1])
    for j in range(out_ref.shape[0]):
        out_ref[j] = rows.astype(bf16)
    sq_ref[...] = jnp.broadcast_to(squares, sq_ref.shape)


def own_place(cols, share):
    group = lax.axis_index("grp")
    per_half = cols // share
    return (group // per_half, pl.multiple_of(group % per_half * share, share))


def pack_body(*refs):
    *sources, out_ref = refs
    share = out_ref.shape[0]
    _, at = own_place(sources[0].shape[0], share)
    sources = [ref.at[pl.ds(at, share)] for ref in sources]
    rights, images, norms = (sources[:ITERS], sources[ITERS : 2 * ITERS], sources[2 * ITERS :])
    width = rights[0].shape[1]
    start_norm = norms[0][:, 0:1]
    phi_bar, rho_bar = (start_norm, norms[0][:, LANES : LANES + 1])
    search, search_image = (rights[0][...], images[0][...])
    coeffs, solution = (jnp.zeros_like(search), jnp.zeros_like(search))
    for k in range(1, ITERS):
        u_norm, next_norm = (norms[k][:, 0:1], norms[k][:, LANES : LANES + 1])
        radius = jnp.sqrt(rho_bar * rho_bar + u_norm * u_norm)
        cosine = rho_bar / radius
        sine_part = u_norm / radius
        coupling = sine_part * next_norm
        rho_bar = -cosine * next_norm
        step = cosine * phi_bar / radius
        phi_bar = sine_part * phi_bar
        coeffs = coeffs + step * search
        solution = solution + step * search_image
        search = rights[k][...] - coupling / radius * search
        search_image = images[k][...] - coupling / radius * search_image
    for j, value in enumerate((coeffs, solution, search, search_image)):
        out_ref[:, j * width : (j + 1) * width] = value
    for j, value in enumerate((phi_bar, rho_bar, start_norm)):
        out_ref[:, 4 * width + j * LANES : 4 * width + (j + 1) * LANES] = jnp.broadcast_to(value, (share, LANES))


def final_body(everyone_ref, mine_ref, twin_ref, out_ref, coeffs_ref, ratio_ref, column):
    share = mine_ref.shape[0]
    width = out_ref.shape[1]
    cols = column.shape[0]
    owner, at = own_place(cols, share)
    sizes = [lax.axis_size(name) for name in every]
    run_length = sizes[3] // 2
    by_half = [jnp.zeros((1, LANES), f32), jnp.zeros((1, LANES), f32)]
    for sender in range(0, everyone_ref.shape[0], run_length):
        line, rest = sender % sizes[3], sender // sizes[3]
        half = int(half_of(rest // 2 % sizes[1], rest % 2 == 1, line, sizes[1], sizes[3]))
        by_half[half] = by_half[half] + jnp.sum(everyone_ref[sender : sender + run_length], axis=0)
    squares = jnp.where(owner == 0, by_half[0], by_half[1])
    column[...] = jnp.broadcast_to(to_column(jnp.sqrt(squares + floor_sq), cols), column.shape)
    u_norm = column[pl.ds(at, share), :][:, 0:1]
    own = owner == own_half()

    def piece(start, length):
        return jnp.where(own, mine_ref[:, start : start + length], twin_ref[:, start : start + length])

    phi_bar, rho_bar, start_norm = (piece(4 * width + j * LANES, LANES)[:, 0:1] for j in range(3))
    radius = jnp.sqrt(rho_bar * rho_bar + u_norm * u_norm)
    step = rho_bar / radius * phi_bar / radius
    phi_bar = u_norm / radius * phi_bar
    coeffs_ref[...] = piece(0, width) + step * piece(2 * width, width)
    out_ref[...] = piece(width, width) + step * piece(3 * width, width)
    ratio_ref[...] = to_lanes(phi_bar / start_norm)[:, :share]


def half_of(x, core, line, x_size, lines):
    far = (2 * x >= x_size) ^ (2 * line >= lines)
    return core ^ far


def own_half():
    return half_of(
        lax.axis_index("x"),
        lax.axis_index("core") == 1,
        lax.axis_index("grp"),
        lax.axis_size("x"),
        lax.axis_size("grp"),
    ).astype(jnp.int32)


def groups_of(kind):
    sizes = [lax.axis_size(name) for name in every]
    groups = {}
    for number, (y, x, core, line) in enumerate(itertools.product(*map(range, sizes))):
        half = half_of(x, core == 1, line, sizes[1], sizes[3])
        key = (line, half) if kind == "plane" else (y, x, half)
        groups.setdefault(key, []).append(number)
    return list(groups.values())


def exchange(tiles, groups=None):
    return lax.all_to_all(tiles, every, 0, 0, axis_index_groups=groups, tiled=True)


def swap_cores(value):
    return lax.ppermute(value, "core", [(0, 1), (1, 0)])


SMALL = 4 * 1024 * 1024


def sum_everywhere(tiles):
    peers, tall, _ = tiles.shape
    kept = tall - SQ_ROWS
    lines = lax.axis_size("grp")
    planes = groups_of("plane")
    (block,) = run(plane_sum_body, [((lines, tall, LANES), bf16)], [exchange(tiles, planes)], [VMEM], "plane_sum", limit=SMALL)
    half, squares = run(
        line_sum_body,
        [((peers, kept, LANES), bf16), ((SQ_ROWS, LANES), f32)],
        [exchange(block, groups_of("line"))],
        [VMEM],
        "line_sum",
        limit=SMALL,
    )
    return (exchange(half, planes), squares)


def shards(matrix, right_side, precond, row_counts):
    local_rows, width = matrix.shape
    cols = right_side.shape[1] // 2
    tiles_shape = (width // LANES, cols + SQ_ROWS, LANES)
    twin_matrix, twin_side, twin_counts = (swap_cores(value) for value in (matrix, right_side, row_counts))
    counts = [row_counts, twin_counts]
    blocks = [matrix, twin_matrix]
    held, turned = run(
        load_body,
        [(precond.shape, bf16), (precond.shape[::-1], bf16)],
        [precond],
        [pl.BlockSpec(memory_space=pltpu.HBM)],
        "load",
        scratch=[pltpu.SemaphoreType.DMA((width // LOAD_ROWS,))],
        limit=36 * 1024 * 1024,
    )
    right_side, turned = lax.optimization_barrier((right_side, turned))
    tiles, residue, turned_own, turned_twin = run(
        start_body,
        [
            (tiles_shape, bf16),
            ((cols, 2 * local_rows), f32),
            (matrix.shape[::-1], bf16),
            (matrix.shape[::-1], bf16),
        ],
        [*counts, right_side, twin_side, *blocks],
        [SMEM] * 2 + [VMEM] * 4,
        "start",
        scratch=[pltpu.VMEM((2 * cols, 2 * local_rows), f32)],
        limit=12 * 1024 * 1024,
    )

    def turn(half, squares, right_vec, residue, last=False):
        first = right_vec is None
        sent = ((lax.axis_size(every), 1, LANES), f32) if last else (tiles_shape, bf16)
        return run(
            functools.partial(turn_body, first, last),
            [sent, (residue.shape, f32), ((cols, width), f32), ((cols, width), f32), ((cols, 2 * LANES), f32)],
            [*counts, half, squares, held, turned, *blocks, turned_own, turned_twin, residue] + ([] if first else [right_vec]),
            [SMEM] * 2 + [VMEM] * (9 if first else 10),
            "turn",
            limit=20 * 1024 * 1024,
        )

    right_vec = None
    rights, images, norms = ([], [], [])
    for turn_index in range(ITERS):
        last = turn_index + 1 == ITERS
        half, squares = sum_everywhere(tiles)
        tiles, residue, right_vec, image, norm_pair = turn(half, squares, right_vec, residue, last)
        rights.append(right_vec)
        images.append(image)
        norms.append(norm_pair)
    everyone = exchange(tiles)
    (tiles,) = run(tiles_body, [(tiles_shape, bf16)], [residue, *blocks], [VMEM] * 3, "tiles", limit=20 * 1024 * 1024)
    half, squares = sum_everywhere(tiles)
    turn(half, squares, right_vec, residue)

    share = 2 * cols // lax.axis_size("grp")
    packed = run(
        pack_body,
        [((share, 4 * width + 3 * LANES), f32)],
        [*rights, *images, *norms],
        [VMEM] * (3 * ITERS),
        "pack",
        limit=12 * 1024 * 1024,
    )[0]
    twin_packed = swap_cores(packed)
    out, coeffs, ratio = run(
        final_body,
        [((share, width), f32), ((share, width), f32), ((1, share), f32)],
        [everyone, packed, twin_packed],
        [VMEM] * 3,
        "final",
        scratch=[pltpu.VMEM((cols, LANES), f32)],
        limit=12 * 1024 * 1024,
    )
    return (out.T, coeffs.T, ratio[0])


def solution(mesh):
    fine = Mesh(mesh.devices.reshape(4, 4, 2, 8), every)
    return jax.shard_map(
        shards,
        mesh=fine,
        in_specs=(P(every, None), P(every, None), P(), P(every)),
        out_specs=(P(None, "grp"), P(None, "grp"), P("grp")),
        check_vma=False,
    )
```

```python
import functools

import jax
import jax.numpy as jnp
from jax import lax
from jax.experimental import pallas as pl
from jax.experimental.pallas import tpu as pltpu
from jax.sharding import Mesh, PartitionSpec as P

ITERS = 3

floor_sq = 0.01
plane = ("y", "x")
every = ("y", "x", "core", "grp")
SQ_ROWS = 8
LANES = 128
LOAD_ROWS = 256
bf16, f32 = jnp.bfloat16, jnp.float32
VMEM = pl.BlockSpec(memory_space=pltpu.VMEM)


def run(body, shapes, operands, specs, name, scratch=(), limit=None):
    return pl.pallas_call(
        body,
        out_shape=[jax.ShapeDtypeStruct(s, t) for s, t in shapes],
        in_specs=specs,
        out_specs=[VMEM] * len(shapes),
        scratch_shapes=list(scratch),
        compiler_params=pltpu.CompilerParams(vmem_limit_bytes=limit),
        name=name,
    )(*operands)


def terms_of(row):
    first = row.astype(bf16).astype(f32)
    second = (row - first).astype(bf16).astype(f32)
    third = (row - first - second).astype(bf16).astype(f32)
    at = lax.broadcasted_iota(jnp.int32, (SQ_ROWS, row.shape[1]), 0)
    return jnp.where(at == 0, first, jnp.where(at == 1, second, jnp.where(at == 2, third, 0.0)))


def to_lanes(column):
    square = jnp.broadcast_to(column, (column.shape[0], LANES))
    spare = jnp.zeros((LANES - column.shape[0], LANES), f32)
    return jnp.concatenate([square, spare]).T[0:1]


def to_column(row, count):
    return jnp.broadcast_to(row, (LANES, LANES)).T[:count, 0:1]


def nn(left, right):
    return jnp.dot(left, right, preferred_element_type=f32)


def squares_of(residue):
    return to_lanes(jnp.sum(residue * residue, axis=1, keepdims=True))


def put_tiles(partial_value, squares, tiles_ref):
    kept = partial_value.shape[0]
    extra = terms_of(squares).astype(bf16)
    for j in range(tiles_ref.shape[0]):
        tiles_ref[j, :kept, :] = partial_value[:, j * LANES : (j + 1) * LANES].astype(bf16)
        tiles_ref[j, kept:, :] = extra


def write_tiles(residue, own_ref, twin_ref, tiles_ref):
    rows = own_ref.shape[0]
    rounded = residue.astype(bf16)
    partial_value = nn(rounded[:, :rows], own_ref[...]) + nn(rounded[:, rows:], twin_ref[...])
    put_tiles(partial_value, squares_of(residue), tiles_ref)


def tiles_body(residue_ref, own_ref, twin_ref, tiles_ref):
    write_tiles(residue_ref[...], own_ref, twin_ref, tiles_ref)


def load_body(source, held, turned, arrived):
    copies = []
    for at in range(0, source.shape[0], LOAD_ROWS):
        block = pl.ds(at, LOAD_ROWS)
        copy = pltpu.make_async_copy(source.at[block], held.at[block], arrived.at[len(copies)])
        copy.start()
        copies.append((copy, at))
    for copy, at in copies:
        copy.wait()
        turned[:, at : at + LOAD_ROWS] = held[at : at + LOAD_ROWS, :].T


def start_body(own_count, twin_count, b_own, b_twin, a_own, a_twin, tiles_ref, residue_ref, live_ref, turned_own, turned_twin, work):
    cols = residue_ref.shape[0]
    rows = b_own.shape[0]
    work[:, :rows] = b_own[...].astype(f32).T
    work[:, rows:] = b_twin[...].astype(f32).T
    mine = work[pl.ds(pl.multiple_of(lax.axis_index("core") * cols, cols), cols), :]
    slot = lax.broadcasted_iota(jnp.int32, (1, rows), 1)
    live = jnp.concatenate([slot < own_count[...], slot < twin_count[...]], axis=1).astype(f32)
    live_ref[...] = live
    residue = live * mine
    residue_ref[...] = residue
    turned_own[...] = a_own[...].T
    turned_twin[...] = a_twin[...].T
    write_tiles(residue, a_own, a_twin, tiles_ref)


def turn_body(first, last, live_ref, half_ref, sq_ref, n_ref, turned_n, a_own, a_twin, turned_own, turned_twin, old_ref, *refs):
    right_ref = None if first else refs[0]
    sent_ref, residue_ref, next_ref, image_ref, norms_ref = refs[-5:]
    cols = half_ref.shape[1]
    u_norm = to_column(jnp.sqrt(sq_ref[0:1] + floor_sq), cols)
    per_u = 1.0 / u_norm
    total = jnp.concatenate([half_ref[j] for j in range(half_ref.shape[0])], axis=1)
    raw_vec = nn(total, n_ref[...]) * per_u
    if not first:
        raw_vec = raw_vec - u_norm * right_ref[...]
    v_norm = jnp.sqrt(jnp.sum(raw_vec * raw_vec, axis=1, keepdims=True) + floor_sq)
    next_vec = raw_vec * (1.0 / v_norm)
    next_ref[...] = next_vec
    image = nn(next_vec.astype(bf16), turned_n[...])
    image_ref[...] = image
    pushed = image.astype(bf16)
    ahead = jnp.concatenate([nn(pushed, turned_own[...]), nn(pushed, turned_twin[...])], axis=1)
    residue = live_ref[...] * (ahead - (v_norm * per_u) * old_ref[...])
    residue_ref[...] = residue
    norms_ref[:, :LANES] = jnp.broadcast_to(u_norm, (cols, LANES))
    norms_ref[:, LANES:] = jnp.broadcast_to(v_norm, (cols, LANES))
    if last:
        sent_ref[...] = jnp.broadcast_to(squares_of(residue).reshape(1, 1, LANES), sent_ref.shape)
    else:
        write_tiles(residue, a_own, a_twin, sent_ref)


def block_sum(tiles_ref, kept):
    total = jnp.sum(tiles_ref[...].astype(f32), axis=0)
    return (total[:kept], jnp.sum(total[kept:], axis=0, keepdims=True))


def plane_sum_body(tiles_ref, out_ref):
    kept = tiles_ref.shape[1] - SQ_ROWS
    rows, squares = block_sum(tiles_ref, kept)
    extra = terms_of(squares).astype(bf16)
    for j in range(out_ref.shape[0]):
        out_ref[j, :kept, :] = rows.astype(bf16)
        out_ref[j, kept:, :] = extra


def line_sum_body(tiles_ref, out_ref, sq_ref):
    rows, squares = block_sum(tiles_ref, out_ref.shape[1])
    for j in range(out_ref.shape[0]):
        out_ref[j] = rows.astype(bf16)
    sq_ref[...] = jnp.broadcast_to(squares, sq_ref.shape)


def own_place(cols, share):
    group = lax.axis_index("grp")
    per_half = cols // share
    return (group // per_half, pl.multiple_of(group % per_half * share, share))


def pack_body(*refs):
    *sources, out_ref = refs
    share = out_ref.shape[0]
    _, at = own_place(sources[0].shape[0], share)
    sources = [ref.at[pl.ds(at, share)] for ref in sources]
    rights, images, norms = (sources[:ITERS], sources[ITERS : 2 * ITERS], sources[2 * ITERS :])
    width = rights[0].shape[1]
    start_norm = norms[0][:, 0:1]
    phi_bar, rho_bar = (start_norm, norms[0][:, LANES : LANES + 1])
    search, search_image = (rights[0][...], images[0][...])
    coeffs, solution = (jnp.zeros_like(search), jnp.zeros_like(search))
    for k in range(1, ITERS):
        u_norm, next_norm = (norms[k][:, 0:1], norms[k][:, LANES : LANES + 1])
        radius = jnp.sqrt(rho_bar * rho_bar + u_norm * u_norm)
        cosine = rho_bar / radius
        sine_part = u_norm / radius
        coupling = sine_part * next_norm
        rho_bar = -cosine * next_norm
        step = cosine * phi_bar / radius
        phi_bar = sine_part * phi_bar
        coeffs = coeffs + step * search
        solution = solution + step * search_image
        search = rights[k][...] - coupling / radius * search
        search_image = images[k][...] - coupling / radius * search_image
    for j, value in enumerate((coeffs, solution, search, search_image)):
        out_ref[:, j * width : (j + 1) * width] = value
    for j, value in enumerate((phi_bar, rho_bar, start_norm)):
        out_ref[:, 4 * width + j * LANES : 4 * width + (j + 1) * LANES] = jnp.broadcast_to(value, (share, LANES))


def final_body(everyone_ref, mine_ref, twin_ref, out_ref, coeffs_ref, ratio_ref, column):
    share = mine_ref.shape[0]
    width = out_ref.shape[1]
    cols = column.shape[0]
    owner, at = own_place(cols, share)
    lines = lax.axis_size("grp")
    by_core = [jnp.zeros((1, LANES), f32), jnp.zeros((1, LANES), f32)]
    for sender in range(0, everyone_ref.shape[0], lines):
        half = sender // lines % 2
        by_core[half] = by_core[half] + jnp.sum(everyone_ref[sender : sender + lines], axis=0)
    squares = jnp.where(owner == 0, by_core[0], by_core[1])
    column[...] = jnp.broadcast_to(to_column(jnp.sqrt(squares + floor_sq), cols), column.shape)
    u_norm = column[pl.ds(at, share), :][:, 0:1]
    own = owner == lax.axis_index("core")

    def piece(start, length):
        return jnp.where(own, mine_ref[:, start : start + length], twin_ref[:, start : start + length])

    phi_bar, rho_bar, start_norm = (piece(4 * width + j * LANES, LANES)[:, 0:1] for j in range(3))
    radius = jnp.sqrt(rho_bar * rho_bar + u_norm * u_norm)
    step = rho_bar / radius * phi_bar / radius
    phi_bar = u_norm / radius * phi_bar
    coeffs_ref[...] = piece(0, width) + step * piece(2 * width, width)
    out_ref[...] = piece(width, width) + step * piece(3 * width, width)
    ratio_ref[...] = to_lanes(phi_bar / start_norm)[:, :share]


def exchange(tiles, axis):
    return lax.all_to_all(tiles, axis, 0, 0, tiled=True)


def swap_cores(value):
    return lax.ppermute(value, "core", [(0, 1), (1, 0)])


SMALL = 4 * 1024 * 1024


def sum_everywhere(tiles):
    peers, tall, _ = tiles.shape
    kept = tall - SQ_ROWS
    lines = lax.axis_size("grp")
    (block,) = run(plane_sum_body, [((lines, tall, LANES), bf16)], [exchange(tiles, plane)], [VMEM], "plane_sum", limit=SMALL)
    half, squares = run(
        line_sum_body,
        [((peers, kept, LANES), bf16), ((SQ_ROWS, LANES), f32)],
        [exchange(block, "grp")],
        [VMEM],
        "line_sum",
        limit=SMALL,
    )
    return (exchange(half, plane), squares)


def shards(matrix, right_side, precond, row_counts):
    local_rows, width = matrix.shape
    cols = right_side.shape[1] // 2
    tiles_shape = (width // LANES, cols + SQ_ROWS, LANES)
    twin_matrix, twin_side, twin_counts = (swap_cores(value) for value in (matrix, right_side, row_counts))
    blocks = [matrix, twin_matrix]
    held, turned = run(
        load_body,
        [(precond.shape, bf16), (precond.shape[::-1], bf16)],
        [precond],
        [pl.BlockSpec(memory_space=pltpu.HBM)],
        "load",
        scratch=[pltpu.SemaphoreType.DMA((width // LOAD_ROWS,))],
        limit=36 * 1024 * 1024,
    )
    counts = [row_counts.reshape(1, 1), twin_counts.reshape(1, 1)]
    right_side, turned = lax.optimization_barrier((right_side, turned))
    tiles, residue, live, turned_own, turned_twin = run(
        start_body,
        [
            (tiles_shape, bf16),
            ((cols, 2 * local_rows), f32),
            ((1, 2 * local_rows), f32),
            (matrix.shape[::-1], bf16),
            (matrix.shape[::-1], bf16),
        ],
        [*counts, right_side, twin_side, *blocks],
        [VMEM] * 6,
        "start",
        scratch=[pltpu.VMEM((2 * cols, 2 * local_rows), f32)],
        limit=12 * 1024 * 1024,
    )

    def turn(half, squares, right_vec, residue, last=False):
        first = right_vec is None
        sent = ((lax.axis_size(every), 1, LANES), f32) if last else (tiles_shape, bf16)
        return run(
            functools.partial(turn_body, first, last),
            [sent, (residue.shape, f32), ((cols, width), f32), ((cols, width), f32), ((cols, 2 * LANES), f32)],
            [live, half, squares, held, turned, *blocks, turned_own, turned_twin, residue] + ([] if first else [right_vec]),
            [VMEM] * (10 if first else 11),
            "turn",
            limit=20 * 1024 * 1024,
        )

    right_vec = None
    rights, images, norms = ([], [], [])
    for turn_index in range(ITERS):
        last = turn_index + 1 == ITERS
        half, squares = sum_everywhere(tiles)
        tiles, residue, right_vec, image, norm_pair = turn(half, squares, right_vec, residue, last)
        rights.append(right_vec)
        images.append(image)
        norms.append(norm_pair)
    everyone = exchange(tiles, every)
    (tiles,) = run(tiles_body, [(tiles_shape, bf16)], [residue, *blocks], [VMEM] * 3, "tiles", limit=20 * 1024 * 1024)
    half, squares = sum_everywhere(tiles)
    turn(half, squares, right_vec, residue)

    share = 2 * cols // lax.axis_size("grp")
    packed = run(
        pack_body,
        [((share, 4 * width + 3 * LANES), f32)],
        [*rights, *images, *norms],
        [VMEM] * (3 * ITERS),
        "pack",
        limit=12 * 1024 * 1024,
    )[0]
    twin_packed = swap_cores(packed)
    out, coeffs, ratio = run(
        final_body,
        [((share, width), f32), ((share, width), f32), ((1, share), f32)],
        [everyone, packed, twin_packed],
        [VMEM] * 3,
        "final",
        scratch=[pltpu.VMEM((cols, LANES), f32)],
        limit=12 * 1024 * 1024,
    )
    return (out.T, coeffs.T, ratio[0])


def solution(mesh):
    fine = Mesh(mesh.devices.reshape(4, 4, 2, 8), every)
    return jax.shard_map(
        shards,
        mesh=fine,
        in_specs=(P(every, None), P(every, None), P(), P(every)),
        out_specs=(P(None, "grp"), P(None, "grp"), P("grp")),
        check_vma=False,
    )
```

```python
import functools

import jax
import jax.numpy as jnp
from jax import lax
from jax.experimental import pallas as pl
from jax.experimental.pallas import tpu as pltpu
from jax.sharding import Mesh, PartitionSpec as P

ITERS = 3

floor_sq = 0.01
plane = ("y", "x")
every = ("y", "x", "core", "grp")
SQ_ROWS = 8
LANES = 128
LOAD_ROWS = 256
bf16, f32 = jnp.bfloat16, jnp.float32
VMEM = pl.BlockSpec(memory_space=pltpu.VMEM)


def run(body, shapes, operands, specs, name, scratch=(), limit=None):
    return pl.pallas_call(
        body,
        out_shape=[jax.ShapeDtypeStruct(s, t) for s, t in shapes],
        in_specs=specs,
        out_specs=[VMEM] * len(shapes),
        scratch_shapes=list(scratch),
        compiler_params=pltpu.CompilerParams(vmem_limit_bytes=limit),
        name=name,
    )(*operands)


def terms_of(row):
    first = row.astype(bf16).astype(f32)
    second = (row - first).astype(bf16).astype(f32)
    third = (row - first - second).astype(bf16).astype(f32)
    at = lax.broadcasted_iota(jnp.int32, (SQ_ROWS, row.shape[1]), 0)
    return jnp.where(at == 0, first, jnp.where(at == 1, second, jnp.where(at == 2, third, 0.0)))


def to_lanes(column):
    square = jnp.broadcast_to(column, (column.shape[0], LANES))
    spare = jnp.zeros((LANES - column.shape[0], LANES), f32)
    return jnp.concatenate([square, spare]).T[0:1]


def to_column(row, count):
    return jnp.broadcast_to(row, (LANES, LANES)).T[:count, 0:1]


def nn(left, right):
    rows = left.shape[0]
    if rows < LANES:
        left = jnp.concatenate([left] * (LANES // rows))
    return jnp.dot(left, right, preferred_element_type=f32)[:rows]


def squares_of(residue):
    return to_lanes(jnp.sum(residue * residue, axis=1, keepdims=True))


def put_tiles(partial_value, squares, tiles_ref):
    kept = partial_value.shape[0]
    extra = terms_of(squares).astype(bf16)
    for j in range(tiles_ref.shape[0]):
        tiles_ref[j, :kept, :] = partial_value[:, j * LANES : (j + 1) * LANES].astype(bf16)
        tiles_ref[j, kept:, :] = extra


def write_tiles(residue, own_ref, twin_ref, tiles_ref):
    rows = own_ref.shape[0]
    rounded = residue.astype(bf16)
    partial_value = nn(rounded[:, :rows], own_ref[...]) + nn(rounded[:, rows:], twin_ref[...])
    put_tiles(partial_value, squares_of(residue), tiles_ref)


def tiles_body(residue_ref, own_ref, twin_ref, tiles_ref):
    write_tiles(residue_ref[...], own_ref, twin_ref, tiles_ref)


def load_body(source, held, turned, arrived):
    copies = []
    for at in range(0, source.shape[0], LOAD_ROWS):
        block = pl.ds(at, LOAD_ROWS)
        copy = pltpu.make_async_copy(source.at[block], held.at[block], arrived.at[len(copies)])
        copy.start()
        copies.append((copy, at))
    for copy, at in copies:
        copy.wait()
        turned[:, at : at + LOAD_ROWS] = held[at : at + LOAD_ROWS, :].T


def start_body(own_count, twin_count, b_own, b_twin, a_own, a_twin, tiles_ref, residue_ref, live_ref, turned_own, turned_twin, work, count, arrived):
    counting = pltpu.make_async_copy(twin_count, count, arrived)
    counting.start()
    cols = residue_ref.shape[0]
    rows = b_own.shape[0]
    work[:, :rows] = b_own[...].astype(f32).T
    work[:, rows:] = b_twin[...].astype(f32).T
    mine = work[pl.ds(pl.multiple_of(lax.axis_index("core") * cols, cols), cols), :]
    turned_own[...] = a_own[...].T
    counting.wait()
    slot = lax.broadcasted_iota(jnp.int32, (1, rows), 1)
    live = jnp.concatenate([slot < own_count[0], slot < count[0]], axis=1).astype(f32)
    live_ref[...] = live
    residue = live * mine
    residue_ref[...] = residue
    turned_twin[...] = a_twin[...].T
    write_tiles(residue, a_own, a_twin, tiles_ref)


def turn_body(first, last, live_ref, half_ref, sq_ref, n_ref, turned_n, a_own, a_twin, turned_own, turned_twin, old_ref, *refs):
    right_ref = None if first else refs[0]
    sent_ref, residue_ref, next_ref, image_ref, norms_ref = refs[-5:]
    cols = half_ref.shape[1]
    u_norm = to_column(jnp.sqrt(sq_ref[0:1] + floor_sq), cols)
    per_u = 1.0 / u_norm
    total = jnp.concatenate([half_ref[j] for j in range(half_ref.shape[0])], axis=1)
    raw_vec = nn(total, n_ref[...]) * per_u
    if not first:
        raw_vec = raw_vec - u_norm * right_ref[...]
    v_norm = jnp.sqrt(jnp.sum(raw_vec * raw_vec, axis=1, keepdims=True) + floor_sq)
    next_vec = raw_vec * (1.0 / v_norm)
    next_ref[...] = next_vec
    image = nn(next_vec.astype(bf16), turned_n[...])
    image_ref[...] = image
    pushed = image.astype(bf16)
    ahead = jnp.concatenate([nn(pushed, turned_own[...]), nn(pushed, turned_twin[...])], axis=1)
    residue = live_ref[...] * (ahead - (v_norm * per_u) * old_ref[...])
    residue_ref[...] = residue
    norms_ref[:, :LANES] = jnp.broadcast_to(u_norm, (cols, LANES))
    norms_ref[:, LANES:] = jnp.broadcast_to(v_norm, (cols, LANES))
    if last:
        sent_ref[...] = jnp.broadcast_to(squares_of(residue).reshape(1, 1, LANES), sent_ref.shape)
    else:
        write_tiles(residue, a_own, a_twin, sent_ref)


def block_sum(tiles_ref, kept):
    total = jnp.sum(tiles_ref[...].astype(f32), axis=0)
    return (total[:kept], jnp.sum(total[kept:], axis=0, keepdims=True))


def plane_sum_body(tiles_ref, out_ref):
    kept = tiles_ref.shape[1] - SQ_ROWS
    rows, squares = block_sum(tiles_ref, kept)
    extra = terms_of(squares).astype(bf16)
    for j in range(out_ref.shape[0]):
        out_ref[j, :kept, :] = rows.astype(bf16)
        out_ref[j, kept:, :] = extra


def line_sum_body(tiles_ref, out_ref, sq_ref):
    rows, squares = block_sum(tiles_ref, out_ref.shape[1])
    for j in range(out_ref.shape[0]):
        out_ref[j] = rows.astype(bf16)
    sq_ref[...] = jnp.broadcast_to(squares, sq_ref.shape)


def own_place(cols, share):
    group = lax.axis_index("grp")
    per_half = cols // share
    return (group // per_half, pl.multiple_of(group % per_half * share, share))


def pack_body(*refs):
    *sources, out_ref = refs
    share = out_ref.shape[0]
    _, at = own_place(sources[0].shape[0], share)
    sources = [ref.at[pl.ds(at, share)] for ref in sources]
    rights, images, norms = (sources[:ITERS], sources[ITERS : 2 * ITERS], sources[2 * ITERS :])
    width = rights[0].shape[1]
    start_norm = norms[0][:, 0:1]
    phi_bar, rho_bar = (start_norm, norms[0][:, LANES : LANES + 1])
    search, search_image = (rights[0][...], images[0][...])
    coeffs, solution = (jnp.zeros_like(search), jnp.zeros_like(search))
    for k in range(1, ITERS):
        u_norm, next_norm = (norms[k][:, 0:1], norms[k][:, LANES : LANES + 1])
        radius = jnp.sqrt(rho_bar * rho_bar + u_norm * u_norm)
        cosine = rho_bar / radius
        sine_part = u_norm / radius
        coupling = sine_part * next_norm
        rho_bar = -cosine * next_norm
        step = cosine * phi_bar / radius
        phi_bar = sine_part * phi_bar
        coeffs = coeffs + step * search
        solution = solution + step * search_image
        search = rights[k][...] - coupling / radius * search
        search_image = images[k][...] - coupling / radius * search_image
    for j, value in enumerate((coeffs, solution, search, search_image)):
        out_ref[:, j * width : (j + 1) * width] = value
    for j, value in enumerate((phi_bar, rho_bar, start_norm)):
        out_ref[:, 4 * width + j * LANES : 4 * width + (j + 1) * LANES] = jnp.broadcast_to(value, (share, LANES))


def final_body(everyone_ref, mine_ref, twin_ref, out_ref, coeffs_ref, ratio_ref, column):
    share = mine_ref.shape[0]
    width = out_ref.shape[1]
    cols = column.shape[0]
    owner, at = own_place(cols, share)
    lines = lax.axis_size("grp")
    by_core = [jnp.zeros((1, LANES), f32), jnp.zeros((1, LANES), f32)]
    for sender in range(0, everyone_ref.shape[0], lines):
        half = sender // lines % 2
        by_core[half] = by_core[half] + jnp.sum(everyone_ref[sender : sender + lines], axis=0)
    squares = jnp.where(owner == 0, by_core[0], by_core[1])
    column[...] = jnp.broadcast_to(to_column(jnp.sqrt(squares + floor_sq), cols), column.shape)
    u_norm = column[pl.ds(at, share), :][:, 0:1]
    own = owner == lax.axis_index("core")

    def piece(start, length):
        return jnp.where(own, mine_ref[:, start : start + length], twin_ref[:, start : start + length])

    phi_bar, rho_bar, start_norm = (piece(4 * width + j * LANES, LANES)[:, 0:1] for j in range(3))
    radius = jnp.sqrt(rho_bar * rho_bar + u_norm * u_norm)
    step = rho_bar / radius * phi_bar / radius
    phi_bar = u_norm / radius * phi_bar
    coeffs_ref[...] = piece(0, width) + step * piece(2 * width, width)
    out_ref[...] = piece(width, width) + step * piece(3 * width, width)
    ratio_ref[...] = to_lanes(phi_bar / start_norm)[:, :share]


def exchange(tiles, axis):
    return lax.all_to_all(tiles, axis, 0, 0, tiled=True)


def swap_cores(value):
    return lax.ppermute(value, "core", [(0, 1), (1, 0)])


SMALL = 4 * 1024 * 1024


def sum_everywhere(tiles):
    peers, tall, _ = tiles.shape
    kept = tall - SQ_ROWS
    lines = lax.axis_size("grp")
    (block,) = run(plane_sum_body, [((lines, tall, LANES), bf16)], [exchange(tiles, plane)], [VMEM], "plane_sum", limit=SMALL)
    half, squares = run(
        line_sum_body,
        [((peers, kept, LANES), bf16), ((SQ_ROWS, LANES), f32)],
        [exchange(block, "grp")],
        [VMEM],
        "line_sum",
        limit=SMALL,
    )
    return (exchange(half, plane), squares)


def shards(matrix, right_side, precond, row_counts):
    local_rows, width = matrix.shape
    cols = right_side.shape[1] // 2
    tiles_shape = (width // LANES, cols + SQ_ROWS, LANES)
    twin_matrix, twin_side, twin_counts = (swap_cores(value) for value in (matrix, right_side, row_counts))
    blocks = [matrix, twin_matrix]
    held, turned = run(
        load_body,
        [(precond.shape, bf16), (precond.shape[::-1], bf16)],
        [precond],
        [pl.BlockSpec(memory_space=pltpu.HBM)],
        "load",
        scratch=[pltpu.SemaphoreType.DMA((width // LOAD_ROWS,))],
        limit=36 * 1024 * 1024,
    )
    right_side, turned = lax.optimization_barrier((right_side, turned))
    tiles, residue, live, turned_own, turned_twin = run(
        start_body,
        [
            (tiles_shape, bf16),
            ((cols, 2 * local_rows), f32),
            ((1, 2 * local_rows), f32),
            (matrix.shape[::-1], bf16),
            (matrix.shape[::-1], bf16),
        ],
        [row_counts, twin_counts, right_side, twin_side, *blocks],
        [pl.BlockSpec(memory_space=pltpu.SMEM), pl.BlockSpec(memory_space=pltpu.HBM)] + [VMEM] * 4,
        "start",
        scratch=[
            pltpu.VMEM((2 * cols, 2 * local_rows), f32),
            pltpu.SMEM((1,), jnp.int32),
            pltpu.SemaphoreType.DMA(()),
        ],
        limit=12 * 1024 * 1024,
    )

    def turn(half, squares, right_vec, residue, last=False):
        first = right_vec is None
        sent = ((lax.axis_size(every), 1, LANES), f32) if last else (tiles_shape, bf16)
        return run(
            functools.partial(turn_body, first, last),
            [sent, (residue.shape, f32), ((cols, width), f32), ((cols, width), f32), ((cols, 2 * LANES), f32)],
            [live, half, squares, held, turned, *blocks, turned_own, turned_twin, residue] + ([] if first else [right_vec]),
            [VMEM] * (10 if first else 11),
            "turn",
            limit=20 * 1024 * 1024,
        )

    right_vec = None
    rights, images, norms = ([], [], [])
    for turn_index in range(ITERS):
        last = turn_index + 1 == ITERS
        half, squares = sum_everywhere(tiles)
        tiles, residue, right_vec, image, norm_pair = turn(half, squares, right_vec, residue, last)
        rights.append(right_vec)
        images.append(image)
        norms.append(norm_pair)
    everyone = exchange(tiles, every)
    (tiles,) = run(tiles_body, [(tiles_shape, bf16)], [residue, *blocks], [VMEM] * 3, "tiles", limit=20 * 1024 * 1024)
    half, squares = sum_everywhere(tiles)
    turn(half, squares, right_vec, residue)

    share = 2 * cols // lax.axis_size("grp")
    packed = run(
        pack_body,
        [((share, 4 * width + 3 * LANES), f32)],
        [*rights, *images, *norms],
        [VMEM] * (3 * ITERS),
        "pack",
        limit=12 * 1024 * 1024,
    )[0]
    twin_packed = swap_cores(packed)
    out, coeffs, ratio = run(
        final_body,
        [((share, width), f32), ((share, width), f32), ((1, share), f32)],
        [everyone, packed, twin_packed],
        [VMEM] * 3,
        "final",
        scratch=[pltpu.VMEM((cols, LANES), f32)],
        limit=12 * 1024 * 1024,
    )
    return (out.T, coeffs.T, ratio[0])


def solution(mesh):
    fine = Mesh(mesh.devices.reshape(4, 4, 2, 8), every)
    return jax.shard_map(
        shards,
        mesh=fine,
        in_specs=(P(every, None), P(every, None), P(), P(every)),
        out_specs=(P(None, "grp"), P(None, "grp"), P("grp")),
        check_vma=False,
    )
```

```python
import functools

import jax
import jax.numpy as jnp
from jax import lax
from jax.experimental import pallas as pl
from jax.experimental.pallas import tpu as pltpu
from jax.sharding import Mesh, PartitionSpec as P

ITERS = 3

floor_sq = 0.01
plane = ("y", "x")
every = ("y", "x", "core", "grp")
SQ_ROWS = 8
LANES = 128
LOAD_ROWS = 256
bf16, f32 = jnp.bfloat16, jnp.float32
VMEM = pl.BlockSpec(memory_space=pltpu.VMEM)


def run(body, shapes, operands, specs, name, scratch=(), limit=None):
    return pl.pallas_call(
        body,
        out_shape=[jax.ShapeDtypeStruct(s, t) for s, t in shapes],
        in_specs=specs,
        out_specs=[VMEM] * len(shapes),
        scratch_shapes=list(scratch),
        compiler_params=pltpu.CompilerParams(vmem_limit_bytes=limit),
        name=name,
    )(*operands)


def terms_of(row):
    first = row.astype(bf16).astype(f32)
    second = (row - first).astype(bf16).astype(f32)
    third = (row - first - second).astype(bf16).astype(f32)
    at = lax.broadcasted_iota(jnp.int32, (SQ_ROWS, row.shape[1]), 0)
    return jnp.where(at == 0, first, jnp.where(at == 1, second, jnp.where(at == 2, third, 0.0)))


def to_lanes(column):
    square = jnp.broadcast_to(column, (column.shape[0], LANES))
    spare = jnp.zeros((LANES - column.shape[0], LANES), f32)
    return jnp.concatenate([square, spare]).T[0:1]


def to_column(row, count):
    return jnp.broadcast_to(row, (LANES, LANES)).T[:count, 0:1]


def nn(left, right):
    rows = left.shape[0]
    if rows < LANES:
        left = jnp.concatenate([left] * (LANES // rows))
    return jnp.dot(left, right, preferred_element_type=f32)[:rows]


def squares_of(residue):
    return to_lanes(jnp.sum(residue * residue, axis=1, keepdims=True))


def put_tiles(partial_value, squares, tiles_ref):
    kept = partial_value.shape[0]
    extra = terms_of(squares).astype(bf16)
    for j in range(tiles_ref.shape[0]):
        tiles_ref[j, :kept, :] = partial_value[:, j * LANES : (j + 1) * LANES].astype(bf16)
        tiles_ref[j, kept:, :] = extra


def write_tiles(residue, own_ref, twin_ref, tiles_ref):
    rows = own_ref.shape[0]
    rounded = residue.astype(bf16)
    partial_value = nn(rounded[:, :rows], own_ref[...]) + nn(rounded[:, rows:], twin_ref[...])
    put_tiles(partial_value, squares_of(residue), tiles_ref)


def tiles_body(residue_ref, own_ref, twin_ref, tiles_ref):
    write_tiles(residue_ref[...], own_ref, twin_ref, tiles_ref)


def load_body(source, held, turned, arrived):
    copies = []
    for at in range(0, source.shape[0], LOAD_ROWS):
        block = pl.ds(at, LOAD_ROWS)
        copy = pltpu.make_async_copy(source.at[block], held.at[block], arrived.at[len(copies)])
        copy.start()
        copies.append((copy, at))
    for copy, at in copies:
        copy.wait()
        turned[:, at : at + LOAD_ROWS] = held[at : at + LOAD_ROWS, :].T


def start_body(own_count, twin_count, b_own, b_twin, a_own, a_twin, tiles_ref, residue_ref, live_ref, turned_own, turned_twin, work, count, arrived):
    counting = pltpu.make_async_copy(twin_count, count, arrived)
    counting.start()
    cols = residue_ref.shape[0]
    rows = b_own.shape[0]
    mine = pl.ds(pl.multiple_of(lax.axis_index("core") * cols, cols), cols)

    def rows_of(count_value, b_ref, a_ref, turned, at):
        work[:, at : at + rows] = b_ref[...].astype(f32).T
        live = (lax.broadcasted_iota(jnp.int32, (1, rows), 1) < count_value).astype(f32)
        live_ref[:, at : at + rows] = live
        residue = live * work[mine, at : at + rows]
        residue_ref[:, at : at + rows] = residue
        turned[...] = a_ref[...].T
        squares = jnp.sum(residue * residue, axis=1, keepdims=True)
        return (nn(residue.astype(bf16), a_ref[...]), squares)

    own_part, own_squares = rows_of(own_count[0], b_own, a_own, turned_own, 0)
    counting.wait()
    twin_part, twin_squares = rows_of(count[0], b_twin, a_twin, turned_twin, rows)
    put_tiles(own_part + twin_part, to_lanes(own_squares + twin_squares), tiles_ref)


def turn_body(first, last, live_ref, half_ref, sq_ref, n_ref, turned_n, a_own, a_twin, turned_own, turned_twin, old_ref, *refs):
    right_ref = None if first else refs[0]
    sent_ref, residue_ref, next_ref, image_ref, norms_ref = refs[-5:]
    cols = half_ref.shape[1]
    u_norm = to_column(jnp.sqrt(sq_ref[0:1] + floor_sq), cols)
    per_u = 1.0 / u_norm
    total = jnp.concatenate([half_ref[j] for j in range(half_ref.shape[0])], axis=1)
    raw_vec = nn(total, n_ref[...]) * per_u
    if not first:
        raw_vec = raw_vec - u_norm * right_ref[...]
    v_norm = jnp.sqrt(jnp.sum(raw_vec * raw_vec, axis=1, keepdims=True) + floor_sq)
    next_vec = raw_vec * (1.0 / v_norm)
    next_ref[...] = next_vec
    image = nn(next_vec.astype(bf16), turned_n[...])
    image_ref[...] = image
    pushed = image.astype(bf16)
    ahead = jnp.concatenate([nn(pushed, turned_own[...]), nn(pushed, turned_twin[...])], axis=1)
    residue = live_ref[...] * (ahead - (v_norm * per_u) * old_ref[...])
    residue_ref[...] = residue
    norms_ref[:, :LANES] = jnp.broadcast_to(u_norm, (cols, LANES))
    norms_ref[:, LANES:] = jnp.broadcast_to(v_norm, (cols, LANES))
    if last:
        sent_ref[...] = jnp.broadcast_to(squares_of(residue).reshape(1, 1, LANES), sent_ref.shape)
    else:
        write_tiles(residue, a_own, a_twin, sent_ref)


def block_sum(tiles_ref, kept):
    total = jnp.sum(tiles_ref[...].astype(f32), axis=0)
    return (total[:kept], jnp.sum(total[kept:], axis=0, keepdims=True))


def plane_sum_body(tiles_ref, out_ref):
    kept = tiles_ref.shape[1] - SQ_ROWS
    rows, squares = block_sum(tiles_ref, kept)
    extra = terms_of(squares).astype(bf16)
    for j in range(out_ref.shape[0]):
        out_ref[j, :kept, :] = rows.astype(bf16)
        out_ref[j, kept:, :] = extra


def line_sum_body(tiles_ref, out_ref, sq_ref):
    rows, squares = block_sum(tiles_ref, out_ref.shape[1])
    for j in range(out_ref.shape[0]):
        out_ref[j] = rows.astype(bf16)
    sq_ref[...] = jnp.broadcast_to(squares, sq_ref.shape)


def own_place(cols, share):
    group = lax.axis_index("grp")
    per_half = cols // share
    return (group // per_half, pl.multiple_of(group % per_half * share, share))


def pack_body(*refs):
    *sources, out_ref = refs
    share = out_ref.shape[0]
    _, at = own_place(sources[0].shape[0], share)
    sources = [ref.at[pl.ds(at, share)] for ref in sources]
    rights, images, norms = (sources[:ITERS], sources[ITERS : 2 * ITERS], sources[2 * ITERS :])
    width = rights[0].shape[1]
    start_norm = norms[0][:, 0:1]
    phi_bar, rho_bar = (start_norm, norms[0][:, LANES : LANES + 1])
    search, search_image = (rights[0][...], images[0][...])
    coeffs, solution = (jnp.zeros_like(search), jnp.zeros_like(search))
    for k in range(1, ITERS):
        u_norm, next_norm = (norms[k][:, 0:1], norms[k][:, LANES : LANES + 1])
        radius = jnp.sqrt(rho_bar * rho_bar + u_norm * u_norm)
        cosine = rho_bar / radius
        sine_part = u_norm / radius
        coupling = sine_part * next_norm
        rho_bar = -cosine * next_norm
        step = cosine * phi_bar / radius
        phi_bar = sine_part * phi_bar
        coeffs = coeffs + step * search
        solution = solution + step * search_image
        search = rights[k][...] - coupling / radius * search
        search_image = images[k][...] - coupling / radius * search_image
    for j, value in enumerate((coeffs, solution, search, search_image)):
        out_ref[:, j * width : (j + 1) * width] = value
    for j, value in enumerate((phi_bar, rho_bar, start_norm)):
        out_ref[:, 4 * width + j * LANES : 4 * width + (j + 1) * LANES] = jnp.broadcast_to(value, (share, LANES))


def final_body(everyone_ref, mine_ref, twin_ref, out_ref, coeffs_ref, ratio_ref, column):
    share = mine_ref.shape[0]
    width = out_ref.shape[1]
    cols = column.shape[0]
    owner, at = own_place(cols, share)
    lines = lax.axis_size("grp")
    by_core = [jnp.zeros((1, LANES), f32), jnp.zeros((1, LANES), f32)]
    for sender in range(0, everyone_ref.shape[0], lines):
        half = sender // lines % 2
        by_core[half] = by_core[half] + jnp.sum(everyone_ref[sender : sender + lines], axis=0)
    squares = jnp.where(owner == 0, by_core[0], by_core[1])
    column[...] = jnp.broadcast_to(to_column(jnp.sqrt(squares + floor_sq), cols), column.shape)
    u_norm = column[pl.ds(at, share), :][:, 0:1]
    own = owner == lax.axis_index("core")

    def piece(start, length):
        return jnp.where(own, mine_ref[:, start : start + length], twin_ref[:, start : start + length])

    phi_bar, rho_bar, start_norm = (piece(4 * width + j * LANES, LANES)[:, 0:1] for j in range(3))
    radius = jnp.sqrt(rho_bar * rho_bar + u_norm * u_norm)
    step = rho_bar / radius * phi_bar / radius
    phi_bar = u_norm / radius * phi_bar
    coeffs_ref[...] = piece(0, width) + step * piece(2 * width, width)
    out_ref[...] = piece(width, width) + step * piece(3 * width, width)
    ratio_ref[...] = to_lanes(phi_bar / start_norm)[:, :share]


def exchange(tiles, axis):
    return lax.all_to_all(tiles, axis, 0, 0, tiled=True)


def swap_cores(value):
    return lax.ppermute(value, "core", [(0, 1), (1, 0)])


SMALL = 4 * 1024 * 1024


def sum_everywhere(tiles):
    peers, tall, _ = tiles.shape
    kept = tall - SQ_ROWS
    lines = lax.axis_size("grp")
    (block,) = run(plane_sum_body, [((lines, tall, LANES), bf16)], [exchange(tiles, plane)], [VMEM], "plane_sum", limit=SMALL)
    half, squares = run(
        line_sum_body,
        [((peers, kept, LANES), bf16), ((SQ_ROWS, LANES), f32)],
        [exchange(block, "grp")],
        [VMEM],
        "line_sum",
        limit=SMALL,
    )
    return (exchange(half, plane), squares)


def shards(matrix, right_side, precond, row_counts):
    local_rows, width = matrix.shape
    cols = right_side.shape[1] // 2
    tiles_shape = (width // LANES, cols + SQ_ROWS, LANES)
    twin_matrix, twin_side, twin_counts = (swap_cores(value) for value in (matrix, right_side, row_counts))
    blocks = [matrix, twin_matrix]
    held, turned = run(
        load_body,
        [(precond.shape, bf16), (precond.shape[::-1], bf16)],
        [precond],
        [pl.BlockSpec(memory_space=pltpu.HBM)],
        "load",
        scratch=[pltpu.SemaphoreType.DMA((width // LOAD_ROWS,))],
        limit=36 * 1024 * 1024,
    )
    right_side, turned = lax.optimization_barrier((right_side, turned))
    tiles, residue, live, turned_own, turned_twin = run(
        start_body,
        [
            (tiles_shape, bf16),
            ((cols, 2 * local_rows), f32),
            ((1, 2 * local_rows), f32),
            (matrix.shape[::-1], bf16),
            (matrix.shape[::-1], bf16),
        ],
        [row_counts, twin_counts, right_side, twin_side, *blocks],
        [pl.BlockSpec(memory_space=pltpu.SMEM), pl.BlockSpec(memory_space=pltpu.HBM)] + [VMEM] * 4,
        "start",
        scratch=[
            pltpu.VMEM((2 * cols, 2 * local_rows), f32),
            pltpu.SMEM((1,), jnp.int32),
            pltpu.SemaphoreType.DMA(()),
        ],
        limit=12 * 1024 * 1024,
    )

    def turn(half, squares, right_vec, residue, last=False):
        first = right_vec is None
        sent = ((lax.axis_size(every), 1, LANES), f32) if last else (tiles_shape, bf16)
        return run(
            functools.partial(turn_body, first, last),
            [sent, (residue.shape, f32), ((cols, width), f32), ((cols, width), f32), ((cols, 2 * LANES), f32)],
            [live, half, squares, held, turned, *blocks, turned_own, turned_twin, residue] + ([] if first else [right_vec]),
            [VMEM] * (10 if first else 11),
            "turn",
            limit=20 * 1024 * 1024,
        )

    right_vec = None
    rights, images, norms = ([], [], [])
    for turn_index in range(ITERS):
        last = turn_index + 1 == ITERS
        half, squares = sum_everywhere(tiles)
        tiles, residue, right_vec, image, norm_pair = turn(half, squares, right_vec, residue, last)
        rights.append(right_vec)
        images.append(image)
        norms.append(norm_pair)
    everyone = exchange(tiles, every)
    (tiles,) = run(tiles_body, [(tiles_shape, bf16)], [residue, *blocks], [VMEM] * 3, "tiles", limit=20 * 1024 * 1024)
    half, squares = sum_everywhere(tiles)
    turn(half, squares, right_vec, residue)

    share = 2 * cols // lax.axis_size("grp")
    packed = run(
        pack_body,
        [((share, 4 * width + 3 * LANES), f32)],
        [*rights, *images, *norms],
        [VMEM] * (3 * ITERS),
        "pack",
        limit=12 * 1024 * 1024,
    )[0]
    twin_packed = swap_cores(packed)
    out, coeffs, ratio = run(
        final_body,
        [((share, width), f32), ((share, width), f32), ((1, share), f32)],
        [everyone, packed, twin_packed],
        [VMEM] * 3,
        "final",
        scratch=[pltpu.VMEM((cols, LANES), f32)],
        limit=12 * 1024 * 1024,
    )
    return (out.T, coeffs.T, ratio[0])


def solution(mesh):
    fine = Mesh(mesh.devices.reshape(4, 4, 2, 8), every)
    return jax.shard_map(
        shards,
        mesh=fine,
        in_specs=(P(every, None), P(every, None), P(), P(every)),
        out_specs=(P(None, "grp"), P(None, "grp"), P("grp")),
        check_vma=False,
    )
```

```python
import functools
import itertools

import jax
import jax.numpy as jnp
from jax import lax
from jax.experimental import pallas as pl
from jax.experimental.pallas import tpu as pltpu
from jax.sharding import Mesh, PartitionSpec as P

ITERS = 3

floor_sq = 0.01
every = ("y", "x", "core", "grp")
SQ_ROWS = 8
LANES = 128
LOAD_ROWS = 256
bf16, f32 = jnp.bfloat16, jnp.float32
VMEM = pl.BlockSpec(memory_space=pltpu.VMEM)


def run(body, shapes, operands, specs, name, scratch=(), limit=None):
    return pl.pallas_call(
        body,
        out_shape=[jax.ShapeDtypeStruct(s, t) for s, t in shapes],
        in_specs=specs,
        out_specs=[VMEM] * len(shapes),
        scratch_shapes=list(scratch),
        compiler_params=pltpu.CompilerParams(vmem_limit_bytes=limit),
        name=name,
    )(*operands)


def terms_of(row):
    first = row.astype(bf16).astype(f32)
    second = (row - first).astype(bf16).astype(f32)
    third = (row - first - second).astype(bf16).astype(f32)
    at = lax.broadcasted_iota(jnp.int32, (SQ_ROWS, row.shape[1]), 0)
    return jnp.where(at == 0, first, jnp.where(at == 1, second, jnp.where(at == 2, third, 0.0)))


def to_lanes(column):
    square = jnp.broadcast_to(column, (column.shape[0], LANES))
    spare = jnp.zeros((LANES - column.shape[0], LANES), f32)
    return jnp.concatenate([square, spare]).T[0:1]


def to_column(row, count):
    return jnp.broadcast_to(row, (LANES, LANES)).T[:count, 0:1]


def nn(left, right):
    rows = left.shape[0]
    if rows < LANES:
        left = jnp.concatenate([left] * (LANES // rows))
    return jnp.dot(left, right, preferred_element_type=f32)[:rows]


def squares_of(residue):
    return to_lanes(jnp.sum(residue * residue, axis=1, keepdims=True))


def put_tiles(partial_value, squares, tiles_ref):
    kept = partial_value.shape[0]
    extra = terms_of(squares).astype(bf16)
    for j in range(tiles_ref.shape[0]):
        tiles_ref[j, :kept, :] = partial_value[:, j * LANES : (j + 1) * LANES].astype(bf16)
        tiles_ref[j, kept:, :] = extra


def write_tiles(residue, own_ref, twin_ref, tiles_ref):
    rows = own_ref.shape[0]
    rounded = residue.astype(bf16)
    partial_value = nn(rounded[:, :rows], own_ref[...]) + nn(rounded[:, rows:], twin_ref[...])
    put_tiles(partial_value, squares_of(residue), tiles_ref)


def tiles_body(residue_ref, own_ref, twin_ref, tiles_ref):
    write_tiles(residue_ref[...], own_ref, twin_ref, tiles_ref)


def load_body(source, held, turned, arrived):
    copies = []
    for at in range(0, source.shape[0], LOAD_ROWS):
        block = pl.ds(at, LOAD_ROWS)
        copy = pltpu.make_async_copy(source.at[block], held.at[block], arrived.at[len(copies)])
        copy.start()
        copies.append((copy, at))
    for copy, at in copies:
        copy.wait()
        turned[:, at : at + LOAD_ROWS] = held[at : at + LOAD_ROWS, :].T


def start_body(own_count, twin_count, b_own, b_twin, a_own, a_twin, tiles_ref, residue_ref, live_ref, turned_own, turned_twin, work, count, arrived):
    counting = pltpu.make_async_copy(twin_count, count, arrived)
    counting.start()
    cols = residue_ref.shape[0]
    rows = b_own.shape[0]
    mine = pl.ds(pl.multiple_of(lax.axis_index("core") * cols, cols), cols)

    def rows_of(count_value, b_ref, a_ref, turned, at):
        work[:, at : at + rows] = b_ref[...].astype(f32).T
        live = (lax.broadcasted_iota(jnp.int32, (1, rows), 1) < count_value).astype(f32)
        live_ref[:, at : at + rows] = live
        residue = live * work[mine, at : at + rows]
        residue_ref[:, at : at + rows] = residue
        turned[...] = a_ref[...].T
        squares = jnp.sum(residue * residue, axis=1, keepdims=True)
        return (nn(residue.astype(bf16), a_ref[...]), squares)

    own_part, own_squares = rows_of(own_count[0], b_own, a_own, turned_own, 0)
    counting.wait()
    twin_part, twin_squares = rows_of(count[0], b_twin, a_twin, turned_twin, rows)
    put_tiles(own_part + twin_part, to_lanes(own_squares + twin_squares), tiles_ref)


def turn_body(first, last, live_ref, half_ref, sq_ref, n_ref, turned_n, a_own, a_twin, turned_own, turned_twin, old_ref, *refs):
    right_ref = None if first else refs[0]
    sent_ref, residue_ref, next_ref, image_ref, norms_ref = refs[-5:]
    cols = half_ref.shape[1]
    u_norm = to_column(jnp.sqrt(sq_ref[0:1] + floor_sq), cols)
    per_u = 1.0 / u_norm
    total = jnp.concatenate([half_ref[j] for j in range(half_ref.shape[0])], axis=1)
    raw_vec = nn(total, n_ref[...]) * per_u
    if not first:
        raw_vec = raw_vec - u_norm * right_ref[...]
    v_norm = jnp.sqrt(jnp.sum(raw_vec * raw_vec, axis=1, keepdims=True) + floor_sq)
    next_vec = raw_vec * (1.0 / v_norm)
    next_ref[...] = next_vec
    image = nn(next_vec.astype(bf16), turned_n[...])
    image_ref[...] = image
    pushed = image.astype(bf16)
    ahead = jnp.concatenate([nn(pushed, turned_own[...]), nn(pushed, turned_twin[...])], axis=1)
    residue = live_ref[...] * (ahead - (v_norm * per_u) * old_ref[...])
    residue_ref[...] = residue
    norms_ref[:, :LANES] = jnp.broadcast_to(u_norm, (cols, LANES))
    norms_ref[:, LANES:] = jnp.broadcast_to(v_norm, (cols, LANES))
    if last:
        sent_ref[...] = jnp.broadcast_to(squares_of(residue).reshape(1, 1, LANES), sent_ref.shape)
    else:
        write_tiles(residue, a_own, a_twin, sent_ref)


def block_sum(tiles_ref, kept):
    total = jnp.sum(tiles_ref[...].astype(f32), axis=0)
    return (total[:kept], jnp.sum(total[kept:], axis=0, keepdims=True))


def plane_sum_body(tiles_ref, out_ref):
    kept = tiles_ref.shape[1] - SQ_ROWS
    rows, squares = block_sum(tiles_ref, kept)
    extra = terms_of(squares).astype(bf16)
    for j in range(out_ref.shape[0]):
        out_ref[j, :kept, :] = rows.astype(bf16)
        out_ref[j, kept:, :] = extra


def line_sum_body(tiles_ref, out_ref, sq_ref):
    rows, squares = block_sum(tiles_ref, out_ref.shape[1])
    for j in range(out_ref.shape[0]):
        out_ref[j] = rows.astype(bf16)
    sq_ref[...] = jnp.broadcast_to(squares, sq_ref.shape)


def own_place(cols, share):
    group = lax.axis_index("grp")
    per_half = cols // share
    return (group // per_half, pl.multiple_of(group % per_half * share, share))


def pack_body(*refs):
    *sources, out_ref = refs
    share = out_ref.shape[0]
    _, at = own_place(sources[0].shape[0], share)
    sources = [ref.at[pl.ds(at, share)] for ref in sources]
    rights, images, norms = (sources[:ITERS], sources[ITERS : 2 * ITERS], sources[2 * ITERS :])
    width = rights[0].shape[1]
    start_norm = norms[0][:, 0:1]
    phi_bar, rho_bar = (start_norm, norms[0][:, LANES : LANES + 1])
    search, search_image = (rights[0][...], images[0][...])
    coeffs, solution = (jnp.zeros_like(search), jnp.zeros_like(search))
    for k in range(1, ITERS):
        u_norm, next_norm = (norms[k][:, 0:1], norms[k][:, LANES : LANES + 1])
        radius = jnp.sqrt(rho_bar * rho_bar + u_norm * u_norm)
        cosine = rho_bar / radius
        sine_part = u_norm / radius
        coupling = sine_part * next_norm
        rho_bar = -cosine * next_norm
        step = cosine * phi_bar / radius
        phi_bar = sine_part * phi_bar
        coeffs = coeffs + step * search
        solution = solution + step * search_image
        search = rights[k][...] - coupling / radius * search
        search_image = images[k][...] - coupling / radius * search_image
    for j, value in enumerate((coeffs, solution, search, search_image)):
        out_ref[:, j * width : (j + 1) * width] = value
    for j, value in enumerate((phi_bar, rho_bar, start_norm)):
        out_ref[:, 4 * width + j * LANES : 4 * width + (j + 1) * LANES] = jnp.broadcast_to(value, (share, LANES))


def final_body(everyone_ref, mine_ref, twin_ref, out_ref, coeffs_ref, ratio_ref, column):
    share = mine_ref.shape[0]
    width = out_ref.shape[1]
    cols = column.shape[0]
    owner, at = own_place(cols, share)
    lines = lax.axis_size("grp")
    by_core = [jnp.zeros((1, LANES), f32), jnp.zeros((1, LANES), f32)]
    for sender in range(0, everyone_ref.shape[0], lines):
        half = sender // lines % 2
        by_core[half] = by_core[half] + jnp.sum(everyone_ref[sender : sender + lines], axis=0)
    squares = jnp.where(owner == 0, by_core[0], by_core[1])
    column[...] = jnp.broadcast_to(to_column(jnp.sqrt(squares + floor_sq), cols), column.shape)
    u_norm = column[pl.ds(at, share), :][:, 0:1]
    own = owner == lax.axis_index("core")

    def piece(start, length):
        return jnp.where(own, mine_ref[:, start : start + length], twin_ref[:, start : start + length])

    phi_bar, rho_bar, start_norm = (piece(4 * width + j * LANES, LANES)[:, 0:1] for j in range(3))
    radius = jnp.sqrt(rho_bar * rho_bar + u_norm * u_norm)
    step = rho_bar / radius * phi_bar / radius
    phi_bar = u_norm / radius * phi_bar
    coeffs_ref[...] = piece(0, width) + step * piece(2 * width, width)
    out_ref[...] = piece(width, width) + step * piece(3 * width, width)
    ratio_ref[...] = to_lanes(phi_bar / start_norm)[:, :share]


def groups_of(kind):
    y_size, x_size, cores, lines = (lax.axis_size(name) for name in every)

    def number(y, x, core, line):
        return ((y * x_size + x) * cores + core) * lines + line

    if kind == "plane":
        steps = itertools.product(range(2), range(2), range(0, x_size, 2), range(0, y_size, 2))
        spots = [(y + up, x + across) for x, y, across, up in steps]
        return [[number(y, x, core, line) for y, x in spots] for core in range(cores) for line in range(lines)]
    spots = [*range(0, lines, 2), *range(lines - 1, 0, -2)]
    planes = itertools.product(range(y_size), range(x_size), range(cores))
    return [[number(y, x, core, line) for line in spots] for y, x, core in planes]


def exchange(tiles, groups=None):
    return lax.all_to_all(tiles, every, 0, 0, axis_index_groups=groups, tiled=True)


def swap_cores(value):
    return lax.ppermute(value, "core", [(0, 1), (1, 0)])


SMALL = 4 * 1024 * 1024


def sum_everywhere(tiles):
    peers, tall, _ = tiles.shape
    kept = tall - SQ_ROWS
    lines = lax.axis_size("grp")
    planes = groups_of("plane")
    (block,) = run(plane_sum_body, [((lines, tall, LANES), bf16)], [exchange(tiles, planes)], [VMEM], "plane_sum", limit=SMALL)
    half, squares = run(
        line_sum_body,
        [((peers, kept, LANES), bf16), ((SQ_ROWS, LANES), f32)],
        [exchange(block, groups_of("line"))],
        [VMEM],
        "line_sum",
        limit=SMALL,
    )
    return (exchange(half, planes), squares)


def shards(matrix, right_side, precond, row_counts):
    local_rows, width = matrix.shape
    cols = right_side.shape[1] // 2
    tiles_shape = (width // LANES, cols + SQ_ROWS, LANES)
    twin_matrix, twin_side, twin_counts = (swap_cores(value) for value in (matrix, right_side, row_counts))
    blocks = [matrix, twin_matrix]
    held, turned = run(
        load_body,
        [(precond.shape, bf16), (precond.shape[::-1], bf16)],
        [precond],
        [pl.BlockSpec(memory_space=pltpu.HBM)],
        "load",
        scratch=[pltpu.SemaphoreType.DMA((width // LOAD_ROWS,))],
        limit=36 * 1024 * 1024,
    )
    right_side, turned = lax.optimization_barrier((right_side, turned))
    tiles, residue, live, turned_own, turned_twin = run(
        start_body,
        [
            (tiles_shape, bf16),
            ((cols, 2 * local_rows), f32),
            ((1, 2 * local_rows), f32),
            (matrix.shape[::-1], bf16),
            (matrix.shape[::-1], bf16),
        ],
        [row_counts, twin_counts, right_side, twin_side, *blocks],
        [pl.BlockSpec(memory_space=pltpu.SMEM), pl.BlockSpec(memory_space=pltpu.HBM)] + [VMEM] * 4,
        "start",
        scratch=[
            pltpu.VMEM((2 * cols, 2 * local_rows), f32),
            pltpu.SMEM((1,), jnp.int32),
            pltpu.SemaphoreType.DMA(()),
        ],
        limit=12 * 1024 * 1024,
    )

    def turn(half, squares, right_vec, residue, last=False):
        first = right_vec is None
        sent = ((lax.axis_size(every), 1, LANES), f32) if last else (tiles_shape, bf16)
        return run(
            functools.partial(turn_body, first, last),
            [sent, (residue.shape, f32), ((cols, width), f32), ((cols, width), f32), ((cols, 2 * LANES), f32)],
            [live, half, squares, held, turned, *blocks, turned_own, turned_twin, residue] + ([] if first else [right_vec]),
            [VMEM] * (10 if first else 11),
            "turn",
            limit=20 * 1024 * 1024,
        )

    right_vec = None
    rights, images, norms = ([], [], [])
    for turn_index in range(ITERS):
        last = turn_index + 1 == ITERS
        half, squares = sum_everywhere(tiles)
        tiles, residue, right_vec, image, norm_pair = turn(half, squares, right_vec, residue, last)
        rights.append(right_vec)
        images.append(image)
        norms.append(norm_pair)
    everyone = exchange(tiles)
    (tiles,) = run(tiles_body, [(tiles_shape, bf16)], [residue, *blocks], [VMEM] * 3, "tiles", limit=20 * 1024 * 1024)
    half, squares = sum_everywhere(tiles)
    turn(half, squares, right_vec, residue)

    share = 2 * cols // lax.axis_size("grp")
    packed = run(
        pack_body,
        [((share, 4 * width + 3 * LANES), f32)],
        [*rights, *images, *norms],
        [VMEM] * (3 * ITERS),
        "pack",
        limit=12 * 1024 * 1024,
    )[0]
    twin_packed = swap_cores(packed)
    out, coeffs, ratio = run(
        final_body,
        [((share, width), f32), ((share, width), f32), ((1, share), f32)],
        [everyone, packed, twin_packed],
        [VMEM] * 3,
        "final",
        scratch=[pltpu.VMEM((cols, LANES), f32)],
        limit=12 * 1024 * 1024,
    )
    return (out.T, coeffs.T, ratio[0])


def solution(mesh):
    fine = Mesh(mesh.devices.reshape(4, 4, 2, 8), every)
    return jax.shard_map(
        shards,
        mesh=fine,
        in_specs=(P(every, None), P(every, None), P(), P(every)),
        out_specs=(P(None, "grp"), P(None, "grp"), P("grp")),
        check_vma=False,
    )
```

```python
import functools

import jax
import jax.numpy as jnp
from jax import lax
from jax.experimental import pallas as pl
from jax.experimental.pallas import tpu as pltpu
from jax.sharding import Mesh, PartitionSpec as P

ITERS = 3

floor_sq = 0.01
plane = ("y", "x")
every = ("y", "x", "core", "grp")
SQ_ROWS = 8
LANES = 128
LOAD_ROWS = 256
bf16, f32 = jnp.bfloat16, jnp.float32
VMEM = pl.BlockSpec(memory_space=pltpu.VMEM)


def run(body, shapes, operands, specs, name, scratch=(), limit=None):
    return pl.pallas_call(
        body,
        out_shape=[jax.ShapeDtypeStruct(s, t) for s, t in shapes],
        in_specs=specs,
        out_specs=[VMEM] * len(shapes),
        scratch_shapes=list(scratch),
        compiler_params=pltpu.CompilerParams(vmem_limit_bytes=limit),
        name=name,
    )(*operands)


def terms_of(row):
    first = row.astype(bf16).astype(f32)
    second = (row - first).astype(bf16).astype(f32)
    third = (row - first - second).astype(bf16).astype(f32)
    at = lax.broadcasted_iota(jnp.int32, (SQ_ROWS, row.shape[1]), 0)
    return jnp.where(at == 0, first, jnp.where(at == 1, second, jnp.where(at == 2, third, 0.0)))


def to_lanes(column):
    square = jnp.broadcast_to(column, (column.shape[0], LANES))
    spare = jnp.zeros((LANES - column.shape[0], LANES), f32)
    return jnp.concatenate([square, spare]).T[0:1]


def to_column(row, count):
    return jnp.broadcast_to(row, (LANES, LANES)).T[:count, 0:1]


def nn(left, right):
    rows = left.shape[0]
    if rows < LANES:
        left = jnp.concatenate([left] * (LANES // rows))
    return jnp.dot(left, right, preferred_element_type=f32)[:rows]


def squares_of(residue):
    return to_lanes(jnp.sum(residue * residue, axis=1, keepdims=True))


def put_tiles(partial_value, squares, tiles_ref):
    kept = partial_value.shape[0]
    extra = terms_of(squares).astype(bf16)
    for j in range(tiles_ref.shape[0]):
        tiles_ref[j, :kept, :] = partial_value[:, j * LANES : (j + 1) * LANES].astype(bf16)
        tiles_ref[j, kept:, :] = extra


def write_tiles(residue, own_ref, twin_ref, tiles_ref):
    rows = own_ref.shape[0]
    rounded = residue.astype(bf16)
    partial_value = nn(rounded[:, :rows], own_ref[...]) + nn(rounded[:, rows:], twin_ref[...])
    put_tiles(partial_value, squares_of(residue), tiles_ref)


def tiles_body(residue_ref, own_ref, twin_ref, tiles_ref):
    write_tiles(residue_ref[...], own_ref, twin_ref, tiles_ref)


def load_body(source, held, turned, arrived):
    copies = []
    for at in range(0, source.shape[0], LOAD_ROWS):
        block = pl.ds(at, LOAD_ROWS)
        copy = pltpu.make_async_copy(source.at[block], held.at[block], arrived.at[len(copies)])
        copy.start()
        copies.append((copy, at))
    for copy, at in copies:
        copy.wait()
        turned[:, at : at + LOAD_ROWS] = held[at : at + LOAD_ROWS, :].T


def start_body(own_count, twin_count, b_own, b_twin, a_own, a_twin, tiles_ref, residue_ref, live_ref, turned_own, turned_twin, work, count, arrived):
    counting = pltpu.make_async_copy(twin_count, count, arrived)
    counting.start()
    cols = residue_ref.shape[0]
    rows = b_own.shape[0]
    mine = pl.ds(pl.multiple_of(lax.axis_index("core") * cols, cols), cols)

    def rows_of(count_value, b_ref, a_ref, turned, at):
        work[:, at : at + rows] = b_ref[...].astype(f32).T
        live = (lax.broadcasted_iota(jnp.int32, (1, rows), 1) < count_value).astype(f32)
        live_ref[:, at : at + rows] = live
        residue = live * work[mine, at : at + rows]
        residue_ref[:, at : at + rows] = residue
        turned[...] = a_ref[...].T
        squares = jnp.sum(residue * residue, axis=1, keepdims=True)
        return (nn(residue.astype(bf16), a_ref[...]), squares)

    own_part, own_squares = rows_of(own_count[0], b_own, a_own, turned_own, 0)
    counting.wait()
    twin_part, twin_squares = rows_of(count[0], b_twin, a_twin, turned_twin, rows)
    put_tiles(own_part + twin_part, to_lanes(own_squares + twin_squares), tiles_ref)


def turn_body(first, last, live_ref, half_ref, sq_ref, n_ref, turned_n, a_own, a_twin, turned_own, turned_twin, old_ref, *refs):
    right_ref = None if first else refs[0]
    sent_ref, residue_ref, next_ref, image_ref, norms_ref = refs[-5:]
    cols = half_ref.shape[1]
    u_norm = to_column(jnp.sqrt(sq_ref[0:1] + floor_sq), cols)
    per_u = 1.0 / u_norm
    total = jnp.concatenate([half_ref[j] for j in range(half_ref.shape[0])], axis=1)
    raw_vec = nn(total, n_ref[...]) * per_u
    if not first:
        raw_vec = raw_vec - u_norm * right_ref[...]
    v_norm = jnp.sqrt(jnp.sum(raw_vec * raw_vec, axis=1, keepdims=True) + floor_sq)
    next_vec = raw_vec * (1.0 / v_norm)
    next_ref[...] = next_vec
    image = nn(next_vec.astype(bf16), turned_n[...])
    image_ref[...] = image
    pushed = image.astype(bf16)
    ahead = jnp.concatenate([nn(pushed, turned_own[...]), nn(pushed, turned_twin[...])], axis=1)
    residue = live_ref[...] * (ahead - (v_norm * per_u) * old_ref[...])
    residue_ref[...] = residue
    norms_ref[:, :LANES] = jnp.broadcast_to(u_norm, (cols, LANES))
    norms_ref[:, LANES:] = jnp.broadcast_to(v_norm, (cols, LANES))
    if last:
        sent_ref[...] = jnp.broadcast_to(squares_of(residue).reshape(1, 1, LANES), sent_ref.shape)
    else:
        write_tiles(residue, a_own, a_twin, sent_ref)


def block_sum(tiles_ref, kept):
    total = jnp.sum(tiles_ref[...].astype(f32), axis=0)
    return (total[:kept], jnp.sum(total[kept:], axis=0, keepdims=True))


def plane_sum_body(tiles_ref, out_ref):
    kept = tiles_ref.shape[1] - SQ_ROWS
    rows, squares = block_sum(tiles_ref, kept)
    extra = terms_of(squares).astype(bf16)
    for j in range(out_ref.shape[0]):
        out_ref[j, :kept, :] = rows.astype(bf16)
        out_ref[j, kept:, :] = extra


def line_sum_body(tiles_ref, out_ref, sq_ref):
    rows, squares = block_sum(tiles_ref, out_ref.shape[1])
    for j in range(out_ref.shape[0]):
        out_ref[j] = rows.astype(bf16)
    sq_ref[...] = jnp.broadcast_to(squares, sq_ref.shape)


def own_place(cols, share):
    group = lax.axis_index("grp")
    per_half = cols // share
    return (group // per_half, pl.multiple_of(group % per_half * share, share))


def pack_body(*refs):
    *sources, out_ref = refs
    share = out_ref.shape[0]
    _, at = own_place(sources[0].shape[0], share)
    sources = [ref.at[pl.ds(at, share)] for ref in sources]
    rights, images, norms = (sources[:ITERS], sources[ITERS : 2 * ITERS], sources[2 * ITERS :])
    width = rights[0].shape[1]
    start_norm = norms[0][:, 0:1]
    phi_bar, rho_bar = (start_norm, norms[0][:, LANES : LANES + 1])
    search, search_image = (rights[0][...], images[0][...])
    coeffs, solution = (jnp.zeros_like(search), jnp.zeros_like(search))
    for k in range(1, ITERS):
        u_norm, next_norm = (norms[k][:, 0:1], norms[k][:, LANES : LANES + 1])
        radius = jnp.sqrt(rho_bar * rho_bar + u_norm * u_norm)
        cosine = rho_bar / radius
        sine_part = u_norm / radius
        coupling = sine_part * next_norm
        rho_bar = -cosine * next_norm
        step = cosine * phi_bar / radius
        phi_bar = sine_part * phi_bar
        coeffs = coeffs + step * search
        solution = solution + step * search_image
        search = rights[k][...] - coupling / radius * search
        search_image = images[k][...] - coupling / radius * search_image
    for j, value in enumerate((coeffs, solution, search, search_image)):
        out_ref[:, j * width : (j + 1) * width] = value
    for j, value in enumerate((phi_bar, rho_bar, start_norm)):
        out_ref[:, 4 * width + j * LANES : 4 * width + (j + 1) * LANES] = jnp.broadcast_to(value, (share, LANES))


def final_body(everyone_ref, mine_ref, twin_ref, out_ref, coeffs_ref, ratio_ref, column):
    share = mine_ref.shape[0]
    width = out_ref.shape[1]
    cols = column.shape[0]
    owner, at = own_place(cols, share)
    lines = lax.axis_size("grp")
    by_core = [jnp.zeros((1, LANES), f32), jnp.zeros((1, LANES), f32)]
    for sender in range(0, everyone_ref.shape[0], lines):
        half = sender // lines % 2
        by_core[half] = by_core[half] + jnp.sum(everyone_ref[sender : sender + lines], axis=0)
    squares = jnp.where(owner == 0, by_core[0], by_core[1])
    column[...] = jnp.broadcast_to(to_column(jnp.sqrt(squares + floor_sq), cols), column.shape)
    u_norm = column[pl.ds(at, share), :][:, 0:1]
    own = owner == lax.axis_index("core")

    def piece(start, length):
        return jnp.where(own, mine_ref[:, start : start + length], twin_ref[:, start : start + length])

    phi_bar, rho_bar, start_norm = (piece(4 * width + j * LANES, LANES)[:, 0:1] for j in range(3))
    radius = jnp.sqrt(rho_bar * rho_bar + u_norm * u_norm)
    step = rho_bar / radius * phi_bar / radius
    phi_bar = u_norm / radius * phi_bar
    coeffs_ref[...] = piece(0, width) + step * piece(2 * width, width)
    out_ref[...] = piece(width, width) + step * piece(3 * width, width)
    ratio_ref[...] = to_lanes(phi_bar / start_norm)[:, :share]


def line_groups():
    y_size, x_size, cores, lines = (lax.axis_size(name) for name in every)
    spots = [*range(0, lines, 2), *range(lines - 1, 0, -2)]
    return [[line * lines + spot for spot in spots] for line in range(y_size * x_size * cores)]


def exchange(tiles, axis, groups=None):
    return lax.all_to_all(tiles, axis, 0, 0, axis_index_groups=groups, tiled=True)


def swap_cores(value):
    return lax.ppermute(value, "core", [(0, 1), (1, 0)])


SMALL = 4 * 1024 * 1024


def sum_everywhere(tiles):
    peers, tall, _ = tiles.shape
    kept = tall - SQ_ROWS
    lines = lax.axis_size("grp")
    (block,) = run(plane_sum_body, [((lines, tall, LANES), bf16)], [exchange(tiles, plane)], [VMEM], "plane_sum", limit=SMALL)
    half, squares = run(
        line_sum_body,
        [((peers, kept, LANES), bf16), ((SQ_ROWS, LANES), f32)],
        [exchange(block, every, line_groups())],
        [VMEM],
        "line_sum",
        limit=SMALL,
    )
    return (exchange(half, plane), squares)


def shards(matrix, right_side, precond, row_counts):
    local_rows, width = matrix.shape
    cols = right_side.shape[1] // 2
    tiles_shape = (width // LANES, cols + SQ_ROWS, LANES)
    twin_matrix, twin_side, twin_counts = (swap_cores(value) for value in (matrix, right_side, row_counts))
    blocks = [matrix, twin_matrix]
    held, turned = run(
        load_body,
        [(precond.shape, bf16), (precond.shape[::-1], bf16)],
        [precond],
        [pl.BlockSpec(memory_space=pltpu.HBM)],
        "load",
        scratch=[pltpu.SemaphoreType.DMA((width // LOAD_ROWS,))],
        limit=36 * 1024 * 1024,
    )
    right_side, turned = lax.optimization_barrier((right_side, turned))
    tiles, residue, live, turned_own, turned_twin = run(
        start_body,
        [
            (tiles_shape, bf16),
            ((cols, 2 * local_rows), f32),
            ((1, 2 * local_rows), f32),
            (matrix.shape[::-1], bf16),
            (matrix.shape[::-1], bf16),
        ],
        [row_counts, twin_counts, right_side, twin_side, *blocks],
        [pl.BlockSpec(memory_space=pltpu.SMEM), pl.BlockSpec(memory_space=pltpu.HBM)] + [VMEM] * 4,
        "start",
        scratch=[
            pltpu.VMEM((2 * cols, 2 * local_rows), f32),
            pltpu.SMEM((1,), jnp.int32),
            pltpu.SemaphoreType.DMA(()),
        ],
        limit=12 * 1024 * 1024,
    )

    def turn(half, squares, right_vec, residue, last=False):
        first = right_vec is None
        sent = ((lax.axis_size(every), 1, LANES), f32) if last else (tiles_shape, bf16)
        return run(
            functools.partial(turn_body, first, last),
            [sent, (residue.shape, f32), ((cols, width), f32), ((cols, width), f32), ((cols, 2 * LANES), f32)],
            [live, half, squares, held, turned, *blocks, turned_own, turned_twin, residue] + ([] if first else [right_vec]),
            [VMEM] * (10 if first else 11),
            "turn",
            limit=20 * 1024 * 1024,
        )

    right_vec = None
    rights, images, norms = ([], [], [])
    for turn_index in range(ITERS):
        last = turn_index + 1 == ITERS
        half, squares = sum_everywhere(tiles)
        tiles, residue, right_vec, image, norm_pair = turn(half, squares, right_vec, residue, last)
        rights.append(right_vec)
        images.append(image)
        norms.append(norm_pair)
    everyone = exchange(tiles, every)
    (tiles,) = run(tiles_body, [(tiles_shape, bf16)], [residue, *blocks], [VMEM] * 3, "tiles", limit=20 * 1024 * 1024)
    half, squares = sum_everywhere(tiles)
    turn(half, squares, right_vec, residue)

    share = 2 * cols // lax.axis_size("grp")
    packed = run(
        pack_body,
        [((share, 4 * width + 3 * LANES), f32)],
        [*rights, *images, *norms],
        [VMEM] * (3 * ITERS),
        "pack",
        limit=12 * 1024 * 1024,
    )[0]
    twin_packed = swap_cores(packed)
    out, coeffs, ratio = run(
        final_body,
        [((share, width), f32), ((share, width), f32), ((1, share), f32)],
        [everyone, packed, twin_packed],
        [VMEM] * 3,
        "final",
        scratch=[pltpu.VMEM((cols, LANES), f32)],
        limit=12 * 1024 * 1024,
    )
    return (out.T, coeffs.T, ratio[0])


def solution(mesh):
    fine = Mesh(mesh.devices.reshape(4, 4, 2, 8), every)
    return jax.shard_map(
        shards,
        mesh=fine,
        in_specs=(P(every, None), P(every, None), P(), P(every)),
        out_specs=(P(None, "grp"), P(None, "grp"), P("grp")),
        check_vma=False,
    )
```
